256 devices in a mesh: groups: 4 (over y, x), expert: 64 (over z, core).
Axes of the slice: x: 2, y: 2, z: 32, core: 2. Of those that a mesh axis runs over, the one named last changes fastest.
The devices are a block of a 4x8x32 slice.
Arguments:
- tokens: bfloat16 [4096, 6144], P(('groups', 'expert')), parts along dimension 0, may hold values from -6 to 6
- route_ids: int32 [4096, 2], P(('groups', 'expert')), parts along dimension 0, may hold values from 0 to 7, all different within a row; in each aligned block of 16 rows (0 to 15, 16 to 31, ...) at most 6 rows name the same one
- route_logits: float32 [4096, 2], P(('groups', 'expert')), parts along dimension 0, may hold values from -6 to 6
- old_place: int32 [64], replicated, may hold values from 0 to 63, each once
- new_place: int32 [64], replicated, may hold values from 0 to 63, each once
- held_gate: bfloat16 [256, 6144, 128], P(('groups', 'expert')), parts along dimension 0, may hold values from -0.078125 to 0.078125
- held_up: bfloat16 [256, 6144, 128], P(('groups', 'expert')), parts along dimension 0, may hold values from -0.078125 to 0.078125
- held_down: bfloat16 [256, 6144, 128], P(('groups', 'expert')), parts along dimension 0, may hold values from -0.1875 to 0.1875
Outputs:
- moe_output: bfloat16 [4096, 6144], P(('groups', 'expert')), parts along dimension 0
- moved_gate: bfloat16 [256, 6144, 128], P(('groups', 'expert')), parts along dimension 0
- moved_up: bfloat16 [256, 6144, 128], P(('groups', 'expert')), parts along dimension 0
- moved_down: bfloat16 [256, 6144, 128], P(('groups', 'expert')), parts along dimension 0
The draws below stay inside these ranges and needn't reach their ends.
There are 4 independent parts, one for each index of `groups`. The reference program is written for one: setup_inputs(seed, part) draws one part's arguments, and reference() takes and returns one part's arrays. A program takes and returns all parts, laid end to end along the dimension named above; an argument that names none is the same for every part. Nothing has to cross between parts.
Inputs may be any that keep to these rules, and one draw needn't show every extreme that they name: `route_ids`: within the rows of one device (aligned blocks of 16 rows) no expert is named by more than 6 rows, a bound that some block reaches; the two ids of a row differ. `old_place`: each device appears once. `new_place`: each device appears once.
All inputs are finite; a program needn't handle non-finite values.
Results may differ from the reference program's by a relative error of at most 0.0058.
Values may be sent and summed in bfloat16 or wider, within the bound.
A program may use at most 128 MiB of HBM per device.

```python
import math
import jax
import jax.numpy as jnp
import numpy as np
from jax import lax

D = 6144
F_SLOT = 128
EXPERTS = 8
TOP = 2
TOK_DEV = 16
CAP = 6
BLOCKS = 8
HIDDEN_SIZE = 1024
TOKENS = 1024
N_EXPERT = 64


def levels(stream_key, shape, pieces, low, top_value):
    gain, own = 1.0, jax.random.fold_in(stream_key, 6)
    for axis_at, shards_of in pieces:
        heights = jnp.exp(jax.random.uniform(jax.random.fold_in(own, axis_at), (shards_of,), jnp.float32, low / len(pieces), top_value / len(pieces)))
        gain = gain * jnp.repeat(heights, shape[axis_at] // shards_of).reshape([-1 if axis == axis_at else 1 for axis in range(len(shape))])
    return gain


def routed_block(key, own, number, rows, count, top, limit, slope):
    sequence = jax.random.permutation(key, count)
    heavy_load, usual = load_shares(count, rows * top, limit, slope, True), load_shares(count, rows * top, limit, slope, False)
    places = jnp.arange(count)

    def named(tallies, rotation):
        used = int((tallies > 0).sum())
        fixed = max(1, used // 4)
        shifted = fixed + (places - fixed + rotation * (used - fixed)) % max(1, count - fixed)
        return jnp.zeros((count,), jnp.int32).at[sequence[jnp.where(places < fixed, places, shifted)]].set(jnp.asarray(tallies, jnp.int32))

    tallies = jnp.where(number % 4 == 0, named(heavy_load, number // 4), named(usual, number - number // 4 - 1))
    mixed = jax.random.permutation(jax.random.fold_in(own, 3), count)
    giver, taker = mixed[0:count // 2 * 2:2], mixed[1:count // 2 * 2:2]
    room = jnp.minimum(tallies[giver] - 1, limit - tallies[taker]) // 2
    room = jnp.where((giver == sequence[0]) | (taker == sequence[0]) | (tallies[taker] == 0), 0, jnp.maximum(room, 0))
    shifted = jax.random.randint(jax.random.fold_in(own, 4), (count // 2,), 0, 1 << 20) % (room + 1)
    tallies = tallies.at[giver].add(-shifted).at[taker].add(shifted)
    items = jnp.searchsorted(jnp.cumsum(tallies), jnp.arange(rows * top), side="right").astype(jnp.int32)
    table = items.reshape(top, rows).T
    table = table[jax.random.permutation(jax.random.fold_in(own, 1), rows)]
    rotation = jax.random.randint(jax.random.fold_in(own, 2), (rows, 1), 0, top)
    return jnp.take_along_axis(table, (jnp.arange(top)[None, :] + rotation) % top, axis=1)


def load_shares(count, total, most, skew, full):
    loads = [(1 << 20) // math.isqrt(rank ** skew) + 1 for rank in range(1, count + 1)]
    largest = most if full else min(most, max(-(-total // count), total * loads[0] // sum(loads)))
    least = 1 if total - largest >= count - 1 else 0
    holding, spare = [largest] + [least] * (count - 1), total - largest - least * (count - 1)
    while spare > 0:
        movable = [i for i in range(1, count) if holding[i] < largest] or [i for i in range(1, count) if holding[i] < most]
        mass, left = sum([loads[i] for i in movable]), spare
        for i in movable:
            extra = min(most - holding[i], max(1, left * loads[i] // mass), spare)
            holding[i] = holding[i] + extra
            spare = spare - extra
    return np.array(holding)


def noise(stream_key, extent, spread, bound, pieces=(), kind=jnp.bfloat16):
    drawn = jax.random.normal(stream_key, extent, jnp.float32) * spread
    if len(pieces) > 0:
        drawn = levels(stream_key, extent, pieces, -0.22, 0.18) * drawn
    return jnp.clip(drawn, min=-bound, max=bound).astype(kind)


def setup_inputs(seed: int = 0, part: int = 0) -> dict:
    streams_of = jax.random.split(jax.random.key(seed), 9)
    part_keys = jax.random.split(jax.random.fold_in(streams_of[8], part), 9)
    tokens = noise(part_keys[0], (TOKENS, D), 1.0, 6.0, ((0, 64),))
    route_ids_keys = jax.random.split(jax.random.fold_in(part_keys[1], 1), TOKENS // TOK_DEV)
    route_ids_turns = jax.random.permutation(jax.random.fold_in(part_keys[1], 3), TOKENS // TOK_DEV)
    route_ids = jax.vmap(lambda own, number: routed_block(jax.random.fold_in(part_keys[1], 2), own, number, TOK_DEV, EXPERTS, TOP, CAP, 2))(route_ids_keys, route_ids_turns).reshape((TOKENS, TOP))
    route_logits = noise(part_keys[2], (TOKENS, TOP), 1.5, 6.0, ((0, 64),), jnp.float32)
    old_place = jax.random.permutation(streams_of[3], N_EXPERT).astype(jnp.int32)
    new_place = jax.random.permutation(streams_of[4], N_EXPERT).astype(jnp.int32)
    held_gate = noise(part_keys[5], (N_EXPERT, D, F_SLOT), D ** -0.5, 0.078125, ((0, 64),))
    held_up = noise(part_keys[6], (N_EXPERT, D, F_SLOT), D ** -0.5, 0.078125, ((0, 64),))
    held_down = noise(part_keys[7], (N_EXPERT, D, F_SLOT), HIDDEN_SIZE ** -0.5, 0.1875, ((0, 64),))
    return dict(tokens=tokens, route_ids=route_ids, route_logits=route_logits, old_place=old_place, new_place=new_place, held_gate=held_gate, held_up=held_up, held_down=held_down)


def reference(tokens, route_ids, route_logits, old_place, new_place, held_gate, held_up, held_down):
    device_ids = jnp.arange(N_EXPERT, dtype=jnp.int32)
    slot_new_at = jnp.sum(jnp.where(new_place[:, None] == device_ids[None, :], device_ids[:, None], 0), axis=0).astype(jnp.int32)
    source_of = jnp.take(old_place, slot_new_at).astype(jnp.int32)
    moved_gate = jnp.take(held_gate, source_of, axis=0)
    moved_up = jnp.take(held_up, source_of, axis=0)
    moved_down = jnp.take(held_down, source_of, axis=0)
    first_weight = 1.0 / (1.0 + jnp.exp(route_logits[:, 1] - route_logits[:, 0]))
    second_weight = 1.0 / (1.0 + jnp.exp(route_logits[:, 0] - route_logits[:, 1]))
    weights = jnp.stack([first_weight, second_weight], axis=1).astype(jnp.float32)
    expert_ids = jnp.arange(EXPERTS, dtype=jnp.int32)
    route_hits = route_ids[:, :, None] == expert_ids[None, None, :]
    coefficient = jnp.sum(jnp.where(route_hits, weights[:, :, None], 0.0), axis=1).astype(jnp.float32)
    routed = jnp.any(route_hits, axis=1)

    def listing(column):
        return jnp.nonzero(column, size=N_EXPERT * CAP, fill_value=TOKENS)[0].astype(jnp.int32)

    index_table = jax.vmap(listing)(routed.T)
    padded_tokens = jnp.concatenate([tokens, jnp.zeros((1, D), jnp.bfloat16)], axis=0)
    padded_coeff = jnp.concatenate([coefficient, jnp.zeros((1, EXPERTS), jnp.float32)], axis=0)

    def apply_slot(slot_index, accumulated):
        expert_index = slot_index // BLOCKS
        row_index = jnp.take(index_table, expert_index, axis=0).astype(jnp.int32)
        slot_rows = jnp.take(padded_tokens, row_index, axis=0)
        holder = jnp.take(old_place, slot_index).astype(jnp.int32)
        w_gate = jnp.take(held_gate, holder, axis=0)
        w_up = jnp.take(held_up, holder, axis=0)
        w_down = jnp.take(held_down, holder, axis=0)
        gate_value = jnp.dot(slot_rows, w_gate, preferred_element_type=jnp.float32)
        up_value = jnp.dot(slot_rows, w_up, preferred_element_type=jnp.float32)
        hidden = (jax.nn.silu(gate_value) * up_value).astype(jnp.bfloat16)
        partial_value = jnp.dot(hidden, w_down.T, preferred_element_type=jnp.float32).astype(jnp.bfloat16)
        partial_value = lax.optimization_barrier(partial_value).astype(jnp.float32)
        scaling = jnp.take(padded_coeff, row_index, axis=0)[:, expert_index]
        return accumulated.at[row_index].add(scaling[:, None] * partial_value)

    start = jnp.zeros((TOKENS + 1, D), jnp.float32)
    summed = lax.fori_loop(0, N_EXPERT, apply_slot, start)
    moe_output = summed[:TOKENS].astype(jnp.bfloat16)
    return moe_output, moved_gate, moved_up, moved_down
```

```python
import functools
import jax
import jax.numpy as jnp
from jax import lax
from jax.experimental import pallas as pl
from jax.experimental.pallas import tpu as pltpu
from jax.sharding import PartitionSpec as P

EXPERTS = 8
CAP = 6
PACKETS = 12
LAG = 2
LANDINGS = 4
SENDS = 3
STAGES = 4
LANES = 128


def plan_kernel(chips, limit, old_ref, new_ref, idx_ref, out_ref, info_ref, rem_v, first_v, sched_v, units_v, sched_s, units_s, queue_s, seen_s, sem):
    slots = 2 * chips
    lane = lax.broadcasted_iota(jnp.int32, (1, LANES), 1)
    upward = lane < chips
    spot = jnp.where(upward, lane, lane - chips)

    def fill(s, carry):
        src, dst = old_ref[s] // 2, new_ref[s] // 2
        ahead = (dst - src + chips) % chips
        back = (chips - ahead) % chips
        origin = jnp.where(upward, src, (chips - src) % chips)
        gone = spot - origin
        gone = jnp.where(gone < 0, gone + chips, gone)
        length = jnp.where(upward, ahead, back)
        here = (lane < slots) & (gone < length)
        rem_v[pl.ds(s, 1), :] = jnp.where(here, length - gone, 0).astype(jnp.float32)
        first_v[pl.ds(s, 1), :] = jnp.where(here & (gone == 0), 1, 0).astype(jnp.float32)
        return carry

    lax.fori_loop(0, slots, fill, 0)
    rem = rem_v[...]
    lanes = lax.broadcasted_iota(jnp.int32, (slots, LANES), 1)
    rows = lax.broadcasted_iota(jnp.int32, (slots, LANES), 0).astype(jnp.float32)
    on = jnp.where(rem > 0, 1.0, 0.0)
    signed = jnp.where(lanes < chips, -on, on)

    def split(i, carry):
        x, beta, step = carry
        share = jnp.where(lanes < chips, x, 1.0 - x)
        load = jnp.sum(share * on, axis=0, keepdims=True)
        top = jnp.max(load, axis=1, keepdims=True)
        price = jnp.where(lane < slots, jnp.exp(beta * (load - top)), 0.0)
        total = jnp.sum(price, axis=1, keepdims=True)
        gain = jnp.sum(signed * price, axis=1, keepdims=True)
        x = jnp.clip(x + step * (gain / total), 0.0, 1.0)
        return x, beta * RISE, step * FALL

    ups = jnp.sum(jnp.where(lanes < chips, on, 0.0), axis=1, keepdims=True)
    x = jnp.clip(0.5 + (0.5 * chips - ups) * 0.25, 0.0, 1.0) * jnp.ones((slots, LANES), jnp.float32)
    x, _, _ = lax.fori_loop(0, ROUNDS, split, (x, jnp.float32(BETA), jnp.float32(STEP)))
    units = jnp.floor(x * PACKETS + 0.5)
    units_v[...] = units.astype(jnp.int32)
    units_copy = pltpu.make_async_copy(units_v, units_s, sem.at[0])
    units_copy.start()
    count = first_v[...] * jnp.where(lanes < chips, units, PACKETS - units)
    key = jnp.where(rem > 0, rem * slots + rows, -3.0)

    def ring(a):
        return jnp.where(spot == 0, pltpu.roll(a, LANES - (chips - 1), 1), pltpu.roll(a, 1, 1))

    def ring_full(a):
        one, wrapped = pltpu.roll(a, 1, 1), pltpu.roll(a, LANES - (chips - 1), 1)
        return jnp.where((lanes == 0) | (lanes == chips), wrapped, one)

    before = jnp.where((rem > 0) & (first_v[...] == 0), ring_full(key), -2.0)
    eight = (8, LANES)

    def step(t, carry):
        count, came, last = carry
        ready = count > 0
        best = jnp.max(jnp.where(ready, key, -1.0), axis=0, keepdims=True)
        sched_v[pl.ds(t, 1), :] = best.astype(jnp.int32)
        count = count - jnp.where(ready & (key == best), 1.0, 0.0) + jnp.where(before == came[0:1], 1.0, 0.0)
        wide = jnp.broadcast_to(best, eight)
        last = jnp.where(wide >= 0, t, last)
        one, wrapped = pltpu.roll(wide, 1, 1), pltpu.roll(wide, LANES - (chips - 1), 1)
        lane8 = lax.broadcasted_iota(jnp.int32, eight, 1)
        return count, jnp.where((lane8 == 0) | (lane8 == chips), wrapped, one), last

    count, came, last = lax.fori_loop(
        0, limit, step, (count, jnp.full(eight, -1.0, jnp.float32), jnp.full(eight, -1, jnp.int32))
    )
    count = count + jnp.where(before == came[0:1], 1.0, 0.0)
    info_ref[0] = (jnp.max(last.astype(jnp.float32)) + 1.0).astype(jnp.int32)
    info_ref[1] = jnp.where(jnp.max(count) > 0, 1, 0)
    sched_copy = pltpu.make_async_copy(sched_v, sched_s, sem.at[1])
    sched_copy.start()
    units_copy.wait()
    sched_copy.wait()

    chip = lax.axis_index("expert") // 2
    mirror = (chips - chip) % chips
    size = slots * PACKETS

    def clear(s, carry):
        for j in range(4):
            seen_s[4 * s + j] = 0

        @pl.when(old_ref[s] // 2 == chip)
        def _():
            base = (old_ref[s] % 2) * PACKETS
            up = units_s[s, 0]
            for p in range(PACKETS):
                queue_s[s * PACKETS + p] = base + p
                queue_s[size + s * PACKETS + p] = base + jnp.minimum(up + p, PACKETS - 1)

        return carry

    lax.fori_loop(0, slots, clear, 0)

    def walk(t, carry):
        for way, (mine, theirs) in enumerate(
            ((chip, (chip + chips - 1) % chips), (chips + mirror, chips + (mirror + chips - 1) % chips))
        ):
            arriving = sched_s[t, theirs]

            @pl.when(arriving >= 0)
            def _():
                s = arriving % slots
                k = seen_s[4 * s + 2 * way]
                queue_s[way * size + s * PACKETS + k] = 2 * PACKETS + 2 * t + way
                seen_s[4 * s + 2 * way] = k + 1

            leaving = sched_s[t, mine]
            s = jnp.maximum(leaving, 0) % slots
            k = seen_s[4 * s + 2 * way + 1]
            idx_ref[2 * t + way] = jnp.where(leaving >= 0, queue_s[way * size + s * PACKETS + jnp.minimum(k, PACKETS - 1)], 0)

            @pl.when(leaving >= 0)
            def _():
                seen_s[4 * s + 2 * way + 1] = k + 1

        return carry

    lax.fori_loop(0, limit, walk, 0)

    def gather(s, carry):
        dst = new_ref[s]

        @pl.when(dst // 2 == chip)
        def _():
            up = jnp.where(old_ref[s] // 2 == chip, PACKETS, units_s[s, 0])
            base = (dst % 2) * PACKETS
            for p in range(PACKETS):
                at = jnp.where(p < up, s * PACKETS + p, size + s * PACKETS + jnp.maximum(p - up, 0))
                out_ref[base + p] = queue_s[at]

        return carry

    lax.fori_loop(0, slots, gather, 0)


ROUNDS = 24
BETA = 2.0 * 0.6931472
STEP = 1.0
RISE = 2.0 ** (1.0 / (ROUNDS - 1))
FALL = 0.05 ** (1.0 / (ROUNDS - 1))


def plan(old_place, new_place, chips, limit):
    slots = 2 * chips
    smem = pl.BlockSpec(memory_space=pltpu.SMEM)
    return pl.pallas_call(
        functools.partial(plan_kernel, chips, limit),
        out_shape=(
            jax.ShapeDtypeStruct((2 * limit,), jnp.int32),
            jax.ShapeDtypeStruct((2 * PACKETS,), jnp.int32),
            jax.ShapeDtypeStruct((2,), jnp.int32),
        ),
        in_specs=[smem, smem],
        out_specs=(smem, smem, smem),
        scratch_shapes=[
            pltpu.VMEM((slots, LANES), jnp.float32),
            pltpu.VMEM((slots, LANES), jnp.float32),
            pltpu.VMEM((limit, LANES), jnp.int32),
            pltpu.VMEM((slots, LANES), jnp.int32),
            pltpu.SMEM((limit, LANES), jnp.int32),
            pltpu.SMEM((slots, LANES), jnp.int32),
            pltpu.SMEM((2 * slots * PACKETS,), jnp.int32),
            pltpu.SMEM((4 * slots,), jnp.int32),
            pltpu.SemaphoreType.DMA((2,)),
        ],
        name="plan",
    )(old_place, new_place)


def move_kernel(chips, steps, per, idx_ref, out_idx_ref, gate, up, down, new_gate, new_up, new_down,
                pool, landing, sending, stage, load_sems, pair_sems, send_sems, recv_sems, stage_sems, out_sems):
    me = lax.axis_index("expert")
    chip, core = me // 2, me % 2
    mate = {"expert": me + 1 - 2 * core}
    above = {"expert": ((chip + 1) % chips) * 2 + core}
    below = {"expert": ((chip + chips - 1) % chips) * 2 + core}
    mesh_ids = pl.DeviceIdType.MESH
    own_arrays = (gate, up, down)
    new_arrays = (new_gate, new_up, new_down)

    barrier = pltpu.get_barrier_semaphore()
    for other in (mate, above, below):
        pl.semaphore_signal(barrier, inc=1, device_id=other, device_id_type=mesh_ids)
    pl.semaphore_wait(barrier, 3)

    loads = []
    for a, array in enumerate(own_arrays):
        given = pltpu.make_async_remote_copy(
            src_ref=array.at[pl.ds((1 - core) * per, per)],
            dst_ref=pool.at[pl.ds(core * PACKETS + a * per, per)],
            send_sem=pair_sems.at[0, a],
            recv_sem=pair_sems.at[1, a],
            device_id=mate,
            device_id_type=mesh_ids,
        )
        given.start()
        kept = pltpu.make_async_copy(
            array.at[pl.ds(core * per, per)], pool.at[pl.ds(core * PACKETS + a * per, per)], load_sems.at[a]
        )
        kept.start()
        loads += [(given, kept)]
    for given, kept in loads:
        kept.wait()
        given.wait()

    def hop(t, way):
        return pltpu.make_async_remote_copy(
            src_ref=sending.at[way, t % SENDS],
            dst_ref=landing.at[way, t % LANDINGS],
            send_sem=send_sems.at[way, t % SENDS],
            recv_sem=recv_sems.at[way, t % LANDINGS],
            device_id=(above, below)[way],
            device_id_type=mesh_ids,
        )

    def take(t):
        for way in range(2):
            hop(t, way).wait_recv()
            pool[2 * PACKETS + 2 * t + way] = landing[way, t % LANDINGS]

    def give(t, free):
        for way in range(2):
            if free:
                hop(t - SENDS, way).wait_send()
            sending[way, t % SENDS] = pool[idx_ref[2 * t + way]]
        for way in range(2):
            hop(t, way).start()

    for t in range(SENDS):
        if t >= LAG:
            take(t - LAG)
        give(t, False)

    def body(t, carry):
        take(t - LAG)
        give(t, True)
        return carry

    lax.fori_loop(SENDS, steps, body, 0)
    for t in range(steps - LAG, steps):
        take(t)
    for t in range(steps - SENDS, steps):
        for way in range(2):
            hop(t, way).wait_send()

    def away(p, slot):
        return pltpu.make_async_remote_copy(
            src_ref=stage.at[1, slot],
            dst_ref=new_arrays[p // per].at[core * per + p % per],
            send_sem=out_sems.at[0, slot],
            recv_sem=out_sems.at[1, p],
            device_id=mate,
            device_id_type=mesh_ids,
        )

    def home(p, slot):
        return pltpu.make_async_copy(
            stage.at[0, slot], new_arrays[p // per].at[core * per + p % per], stage_sems.at[slot]
        )

    for p in range(PACKETS):
        slot = p % STAGES
        if p >= STAGES:
            home(p - STAGES, slot).wait()
            away(p - STAGES, slot).wait_send()
        stage[0, slot] = pool[out_idx_ref[core * PACKETS + p]]
        stage[1, slot] = pool[out_idx_ref[(1 - core) * PACKETS + p]]
        home(p, slot).start()
        away(p, slot).start()
    for p in range(PACKETS - STAGES, PACKETS):
        home(p, p % STAGES).wait()
        away(p, p % STAGES).wait_send()
    for p in range(PACKETS):
        away(p, p % STAGES).wait_recv()


def move(idx, out_idx, gate, up, down, chips, steps, collective_id):
    wide, feats = gate.shape[1], gate.shape[2]
    per = PACKETS // 3
    rows = wide // (2 * per)
    packet = (rows, feats)
    cut = (2 * per, rows, feats)
    any_space = pl.BlockSpec(memory_space=pl.ANY)
    smem = pl.BlockSpec(memory_space=pltpu.SMEM)
    out = jax.ShapeDtypeStruct(cut, gate.dtype)
    dma = pltpu.SemaphoreType.DMA
    moved = pl.pallas_call(
        functools.partial(move_kernel, chips, steps, per),
        out_shape=(out, out, out),
        in_specs=[smem, smem, any_space, any_space, any_space],
        out_specs=(any_space, any_space, any_space),
        scratch_shapes=[
            pltpu.VMEM((2 * PACKETS + 2 * steps,) + packet, gate.dtype),
            pltpu.VMEM((2, LANDINGS) + packet, gate.dtype),
            pltpu.VMEM((2, SENDS) + packet, gate.dtype),
            pltpu.VMEM((2, STAGES) + packet, gate.dtype),
            dma((3,)),
            dma((2, 3)),
            dma((2, SENDS)),
            dma((2, LANDINGS)),
            dma((STAGES,)),
            dma((2, PACKETS)),
        ],
        compiler_params=pltpu.CompilerParams(
            collective_id=collective_id, has_side_effects=True, vmem_limit_bytes=67043328
        ),
        name="move",
    )(idx, out_idx, gate.reshape(cut), up.reshape(cut), down.reshape(cut))
    return tuple(m.reshape(gate.shape) for m in moved)


def in_one_piece(arrays, axis, split_dim, concat_dim, along):
    both = jnp.concatenate(arrays, axis=along)
    out, at, gathered = (
        lax.all_to_all(both, axis, split_axis=split_dim, concat_axis=concat_dim, tiled=True),
        0,
        [],
    )
    for a in arrays:
        gathered.append(lax.slice_in_dim(out, at, at + a.shape[along], axis=along))
        at += a.shape[along]
    return tuple(gathered)


LIMIT = 144
STEPS = (108, 116, 124, 132, 144)


def two_exchanges(source_of, held_gate, held_up, held_down):
    pieces = in_one_piece((held_gate, held_up, held_down), "expert", 1, 0, 2)
    reordered = tuple(jnp.take(p, source_of, axis=0) for p in pieces)
    return in_one_piece(reordered, "expert", 0, 1, 2)


def migrate(old_place, new_place, slot_new_at, held_gate, held_up, held_down):
    chips = lax.axis_size("expert") // 2
    source_of = jnp.take(old_place, slot_new_at)
    idx, out_idx, info = plan(old_place, new_place, chips, LIMIT)
    fits = [(info[0] <= s) & (info[1] == 0) for s in STEPS]
    choice = len(STEPS) - sum(f.astype(jnp.int32) for f in fits)
    branches = [
        functools.partial(lambda s, i, args: move(args[0], args[1], args[2], args[3], args[4], chips, s, i), s, i)
        for i, s in enumerate(STEPS)
    ]
    branches.append(lambda args: two_exchanges(source_of, args[2], args[3], args[4]))
    return lax.switch(choice, branches, (idx, out_idx, held_gate, held_up, held_down))


def inverse_of(placement, device_ids):
    return jnp.sum(
        jnp.where(placement[:, None] == device_ids[None, :], device_ids[:, None], 0), axis=0
    )


def per_device(
    tokens, route_ids, route_logits, old_place, new_place, held_gate, held_up, held_down
):
    devices = lax.axis_size("expert")
    width = tokens.shape[1]
    tok_rows = tokens.shape[0]
    device_ids = jnp.arange(devices, dtype=jnp.int32)
    slot_new_at = inverse_of(new_place, device_ids)
    slot_old_at = inverse_of(old_place, device_ids)
    moved = migrate(old_place, new_place, slot_new_at, held_gate, held_up, held_down)
    w_gate, w_up, w_down = (held_gate, held_up, held_down)
    blocks = devices // EXPERTS
    expert_at = slot_old_at // blocks
    expert_ids = jnp.arange(EXPERTS, dtype=jnp.int32)
    route_hits = route_ids[:, :, None] == expert_ids[None, None, :]
    routed = jnp.any(route_hits, axis=1).astype(jnp.int32)
    position = jnp.cumsum(routed, axis=0) - 1
    bucket_ids = jnp.arange(CAP, dtype=jnp.int32)
    bucket_table = (routed[:, :, None] == 1) & (position[:, :, None] == bucket_ids[None, None, :])
    picker = bucket_table.reshape(tok_rows, EXPERTS * CAP).astype(jnp.bfloat16)
    buckets = lax.dot_general(
        picker, tokens, (((0,), (0,)), ((), ())), preferred_element_type=jnp.float32
    )
    buckets = buckets.astype(jnp.bfloat16).reshape(EXPERTS, CAP, width)
    outgoing = jnp.take(buckets, expert_at, axis=0)
    incoming = lax.all_to_all(outgoing, "expert", split_axis=0, concat_axis=0, tiled=True)
    sources = incoming.shape[0]
    count = incoming.shape[1]
    stacked = incoming.reshape(sources * count, width)
    gate_value = jnp.dot(stacked, w_gate[0], preferred_element_type=jnp.float32)
    up_value = jnp.dot(stacked, w_up[0], preferred_element_type=jnp.float32)
    hidden = (jax.nn.silu(gate_value) * up_value).astype(jnp.bfloat16)
    partial_value = lax.dot_general(
        hidden, w_down[0], (((1,), (1,)), ((), ())), preferred_element_type=jnp.float32
    )
    partial_value = partial_value.astype(jnp.bfloat16).reshape(sources, count, width)
    returned = lax.all_to_all(partial_value, "expert", split_axis=0, concat_axis=0, tiled=True)
    membership = (expert_at[None, :] == expert_ids[:, None]).astype(jnp.bfloat16)
    expert_sum = jnp.dot(
        membership, returned.reshape(devices, CAP * width), preferred_element_type=jnp.float32
    )
    expert_sum = expert_sum.reshape(EXPERTS * CAP, width)
    token_slot = jnp.take_along_axis(position, route_ids, axis=1)
    row_index = route_ids * CAP + token_slot
    selected = jnp.take(expert_sum, row_index.reshape(-1), axis=0).reshape(tok_rows, 2, width)
    first_weight = 1.0 / (1.0 + jnp.exp(route_logits[:, 1] - route_logits[:, 0]))
    second_weight = 1.0 / (1.0 + jnp.exp(route_logits[:, 0] - route_logits[:, 1]))
    weights = jnp.stack([first_weight, second_weight], axis=1)
    combined = jnp.sum(weights[:, :, None] * selected, axis=1).astype(jnp.bfloat16)
    return (combined, moved[0], moved[1], moved[2])


def solution(mesh):
    placed = (
        P(("groups", "expert"), None),
        P(("groups", "expert"), None),
        P(("groups", "expert"), None),
        P(),
        P(),
        P(("groups", "expert"), None, None),
        P(("groups", "expert"), None, None),
        P(("groups", "expert"), None, None),
    )
    return jax.shard_map(
        per_device,
        mesh=mesh,
        in_specs=placed,
        out_specs=(
            P(("groups", "expert"), None),
            P(("groups", "expert"), None, None),
            P(("groups", "expert"), None, None),
            P(("groups", "expert"), None, None),
        ),
        check_vma=False,
    )
```

```python
import functools
import jax
import jax.numpy as jnp
from jax import lax
from jax.experimental import pallas as pl
from jax.experimental.pallas import tpu as pltpu
from jax.sharding import PartitionSpec as P

EXPERTS = 8
CAP = 6
PACKETS = 12
LAG = 2
LANDINGS = 4
SENDS = 3
STAGES = 4
LANES = 128


def plan_kernel(chips, limit, old_ref, new_ref, idx_ref, out_ref, info_ref, rem_v, first_v, sched_v, units_v, sched_s, units_s, queue_s, seen_s, sem):
    slots = 2 * chips
    lane = lax.broadcasted_iota(jnp.int32, (1, LANES), 1)
    upward = lane < chips
    spot = jnp.where(upward, lane, lane - chips)

    def fill(s, carry):
        src, dst = old_ref[s] // 2, new_ref[s] // 2
        ahead = (dst - src + chips) % chips
        back = (chips - ahead) % chips
        origin = jnp.where(upward, src, (chips - src) % chips)
        gone = spot - origin
        gone = jnp.where(gone < 0, gone + chips, gone)
        length = jnp.where(upward, ahead, back)
        here = (lane < slots) & (gone < length)
        rem_v[pl.ds(s, 1), :] = jnp.where(here, length - gone, 0).astype(jnp.float32)
        first_v[pl.ds(s, 1), :] = jnp.where(here & (gone == 0), 1, 0).astype(jnp.float32)
        return carry

    lax.fori_loop(0, slots, fill, 0)
    rem = rem_v[...]
    lanes = lax.broadcasted_iota(jnp.int32, (slots, LANES), 1)
    rows = lax.broadcasted_iota(jnp.int32, (slots, LANES), 0).astype(jnp.float32)
    on = jnp.where(rem > 0, 1.0, 0.0)
    signed = jnp.where(lanes < chips, -on, on)

    def split(i, carry):
        x, beta, step = carry
        share = jnp.where(lanes < chips, x, 1.0 - x)
        load = jnp.sum(share * on, axis=0, keepdims=True)
        top = jnp.max(load, axis=1, keepdims=True)
        price = jnp.where(lane < slots, jnp.exp(beta * (load - top)), 0.0)
        total = jnp.sum(price, axis=1, keepdims=True)
        gain = jnp.sum(signed * price, axis=1, keepdims=True)
        x = jnp.clip(x + step * (gain / total), 0.0, 1.0)
        return x, beta * RISE, step * FALL

    ups = jnp.sum(jnp.where(lanes < chips, on, 0.0), axis=1, keepdims=True)
    x = jnp.clip(0.5 + (0.5 * chips - ups) * 0.25, 0.0, 1.0) * jnp.ones((slots, LANES), jnp.float32)
    x, _, _ = lax.fori_loop(0, ROUNDS, split, (x, jnp.float32(BETA), jnp.float32(STEP)))
    units = jnp.floor(x * PACKETS + 0.5)
    units_v[...] = units.astype(jnp.int32)
    units_copy = pltpu.make_async_copy(units_v, units_s, sem.at[0])
    units_copy.start()
    count = first_v[...] * jnp.where(lanes < chips, units, PACKETS - units)
    key = jnp.where(rem > 0, rem * slots + rows, -3.0)

    def ring(a):
        return jnp.where(spot == 0, pltpu.roll(a, LANES - (chips - 1), 1), pltpu.roll(a, 1, 1))

    def ring_full(a):
        one, wrapped = pltpu.roll(a, 1, 1), pltpu.roll(a, LANES - (chips - 1), 1)
        return jnp.where((lanes == 0) | (lanes == chips), wrapped, one)

    before = jnp.where((rem > 0) & (first_v[...] == 0), ring_full(key), -2.0)
    eight = (8, LANES)

    def step(t, carry):
        count, came, last = carry
        ready = count > 0
        best = jnp.max(jnp.where(ready, key, -1.0), axis=0, keepdims=True)
        sched_v[pl.ds(t, 1), :] = best.astype(jnp.int32)
        count = count - jnp.where(ready & (key == best), 1.0, 0.0) + jnp.where(before == came[0:1], 1.0, 0.0)
        wide = jnp.broadcast_to(best, eight)
        last = jnp.where(wide >= 0, t, last)
        one, wrapped = pltpu.roll(wide, 1, 1), pltpu.roll(wide, LANES - (chips - 1), 1)
        lane8 = lax.broadcasted_iota(jnp.int32, eight, 1)
        return count, jnp.where((lane8 == 0) | (lane8 == chips), wrapped, one), last

    count, came, last = lax.fori_loop(
        0, limit, step, (count, jnp.full(eight, -1.0, jnp.float32), jnp.full(eight, -1, jnp.int32))
    )
    count = count + jnp.where(before == came[0:1], 1.0, 0.0)
    info_ref[0] = (jnp.max(last.astype(jnp.float32)) + 1.0).astype(jnp.int32)
    info_ref[1] = jnp.where(jnp.max(count) > 0, 1, 0)
    sched_copy = pltpu.make_async_copy(sched_v, sched_s, sem.at[1])
    sched_copy.start()
    units_copy.wait()
    sched_copy.wait()

    chip = lax.axis_index("expert") // 2
    mirror = (chips - chip) % chips
    size = slots * PACKETS

    def clear(s, carry):
        for j in range(4):
            seen_s[4 * s + j] = 0

        @pl.when(old_ref[s] // 2 == chip)
        def _():
            base = (old_ref[s] % 2) * PACKETS
            up = units_s[s, 0]
            for p in range(PACKETS):
                queue_s[s * PACKETS + p] = base + p
                queue_s[size + s * PACKETS + p] = base + jnp.minimum(up + p, PACKETS - 1)

        return carry

    lax.fori_loop(0, slots, clear, 0)

    def walk(t, carry):
        for way, (mine, theirs) in enumerate(
            ((chip, (chip + chips - 1) % chips), (chips + mirror, chips + (mirror + chips - 1) % chips))
        ):
            arriving = sched_s[t, theirs]

            @pl.when(arriving >= 0)
            def _():
                s = arriving % slots
                k = seen_s[4 * s + 2 * way]
                queue_s[way * size + s * PACKETS + k] = 2 * PACKETS + 2 * t + way
                seen_s[4 * s + 2 * way] = k + 1

            leaving = sched_s[t, mine]
            s = jnp.maximum(leaving, 0) % slots
            k = seen_s[4 * s + 2 * way + 1]
            idx_ref[2 * t + way] = jnp.where(leaving >= 0, queue_s[way * size + s * PACKETS + jnp.minimum(k, PACKETS - 1)], 0)

            @pl.when(leaving >= 0)
            def _():
                seen_s[4 * s + 2 * way + 1] = k + 1

        return carry

    lax.fori_loop(0, limit, walk, 0)

    def gather(s, carry):
        dst = new_ref[s]

        @pl.when(dst // 2 == chip)
        def _():
            up = jnp.where(old_ref[s] // 2 == chip, PACKETS, units_s[s, 0])
            base = (dst % 2) * PACKETS
            for p in range(PACKETS):
                at = jnp.where(p < up, s * PACKETS + p, size + s * PACKETS + jnp.maximum(p - up, 0))
                out_ref[base + p] = queue_s[at]

        return carry

    lax.fori_loop(0, slots, gather, 0)


ROUNDS = 24
BETA = 2.0 * 0.6931472
STEP = 1.0
RISE = 2.0 ** (1.0 / (ROUNDS - 1))
FALL = 0.05 ** (1.0 / (ROUNDS - 1))


def plan(old_place, new_place, chips, limit):
    slots = 2 * chips
    smem = pl.BlockSpec(memory_space=pltpu.SMEM)
    return pl.pallas_call(
        functools.partial(plan_kernel, chips, limit),
        out_shape=(
            jax.ShapeDtypeStruct((2 * limit,), jnp.int32),
            jax.ShapeDtypeStruct((2 * PACKETS,), jnp.int32),
            jax.ShapeDtypeStruct((2,), jnp.int32),
        ),
        in_specs=[smem, smem],
        out_specs=(smem, smem, smem),
        scratch_shapes=[
            pltpu.VMEM((slots, LANES), jnp.float32),
            pltpu.VMEM((slots, LANES), jnp.float32),
            pltpu.VMEM((limit, LANES), jnp.int32),
            pltpu.VMEM((slots, LANES), jnp.int32),
            pltpu.SMEM((limit, LANES), jnp.int32),
            pltpu.SMEM((slots, LANES), jnp.int32),
            pltpu.SMEM((2 * slots * PACKETS,), jnp.int32),
            pltpu.SMEM((4 * slots,), jnp.int32),
            pltpu.SemaphoreType.DMA((2,)),
        ],
        name="plan",
    )(old_place, new_place)


def move_kernel(chips, steps, per, idx_ref, out_idx_ref, gate, up, down, new_gate, new_up, new_down,
                pool, landing, sending, stage, load_sems, pair_sems, send_sems, recv_sems, stage_sems, out_sems):
    me = lax.axis_index("expert")
    chip, core = me // 2, me % 2
    mate = {"expert": me + 1 - 2 * core}
    above = {"expert": ((chip + 1) % chips) * 2 + core}
    below = {"expert": ((chip + chips - 1) % chips) * 2 + core}
    mesh_ids = pl.DeviceIdType.MESH
    own_arrays = (gate, up, down)
    new_arrays = (new_gate, new_up, new_down)

    barrier = pltpu.get_barrier_semaphore()
    for other in (mate, above, below):
        pl.semaphore_signal(barrier, inc=1, device_id=other, device_id_type=mesh_ids)
    pl.semaphore_wait(barrier, 3)

    loads = []
    for a, array in enumerate(own_arrays):
        given = pltpu.make_async_remote_copy(
            src_ref=array.at[pl.ds((1 - core) * per, per)],
            dst_ref=pool.at[pl.ds(core * PACKETS + a * per, per)],
            send_sem=pair_sems.at[0, a],
            recv_sem=pair_sems.at[1, a],
            device_id=mate,
            device_id_type=mesh_ids,
        )
        given.start()
        kept = pltpu.make_async_copy(
            array.at[pl.ds(core * per, per)], pool.at[pl.ds(core * PACKETS + a * per, per)], load_sems.at[a]
        )
        kept.start()
        loads += [(given, kept)]
    for given, kept in loads:
        kept.wait()
        given.wait()

    def hop(t, way):
        return pltpu.make_async_remote_copy(
            src_ref=sending.at[way, t % SENDS],
            dst_ref=landing.at[way, t % LANDINGS],
            send_sem=send_sems.at[way, t % SENDS],
            recv_sem=recv_sems.at[way, t % LANDINGS],
            device_id=(above, below)[way],
            device_id_type=mesh_ids,
        )

    def take(t):
        for way in range(2):
            hop(t, way).wait_recv()
            pool[2 * PACKETS + 2 * t + way] = landing[way, t % LANDINGS]

    def give(t, free):
        for way in range(2):
            if free:
                hop(t - SENDS, way).wait_send()
            sending[way, t % SENDS] = pool[idx_ref[2 * t + way]]
        for way in range(2):
            hop(t, way).start()

    for t in range(SENDS):
        if t >= LAG:
            take(t - LAG)
        give(t, False)

    def body(t, carry):
        take(t - LAG)
        give(t, True)
        return carry

    lax.fori_loop(SENDS, steps, body, 0)
    for t in range(steps - LAG, steps):
        take(t)
    for t in range(steps - SENDS, steps):
        for way in range(2):
            hop(t, way).wait_send()

    def away(p, slot):
        return pltpu.make_async_remote_copy(
            src_ref=stage.at[1, slot],
            dst_ref=new_arrays[p // per].at[core * per + p % per],
            send_sem=out_sems.at[0, slot],
            recv_sem=out_sems.at[1, p],
            device_id=mate,
            device_id_type=mesh_ids,
        )

    def home(p, slot):
        return pltpu.make_async_copy(
            stage.at[0, slot], new_arrays[p // per].at[core * per + p % per], stage_sems.at[slot]
        )

    for p in range(PACKETS):
        slot = p % STAGES
        if p >= STAGES:
            home(p - STAGES, slot).wait()
            away(p - STAGES, slot).wait_send()
        stage[0, slot] = pool[out_idx_ref[core * PACKETS + p]]
        stage[1, slot] = pool[out_idx_ref[(1 - core) * PACKETS + p]]
        home(p, slot).start()
        away(p, slot).start()
    for p in range(PACKETS - STAGES, PACKETS):
        home(p, p % STAGES).wait()
        away(p, p % STAGES).wait_send()
    for p in range(PACKETS):
        away(p, p % STAGES).wait_recv()


def move(idx, out_idx, gate, up, down, chips, steps, collective_id):
    wide, feats = gate.shape[1], gate.shape[2]
    per = PACKETS // 3
    rows = wide // (2 * per)
    packet = (rows, feats)
    cut = (2 * per, rows, feats)
    any_space = pl.BlockSpec(memory_space=pl.ANY)
    smem = pl.BlockSpec(memory_space=pltpu.SMEM)
    out = jax.ShapeDtypeStruct(cut, gate.dtype)
    dma = pltpu.SemaphoreType.DMA
    moved = pl.pallas_call(
        functools.partial(move_kernel, chips, steps, per),
        out_shape=(out, out, out),
        in_specs=[smem, smem, any_space, any_space, any_space],
        out_specs=(any_space, any_space, any_space),
        scratch_shapes=[
            pltpu.VMEM((2 * PACKETS + 2 * steps,) + packet, gate.dtype),
            pltpu.VMEM((2, LANDINGS) + packet, gate.dtype),
            pltpu.VMEM((2, SENDS) + packet, gate.dtype),
            pltpu.VMEM((2, STAGES) + packet, gate.dtype),
            dma((3,)),
            dma((2, 3)),
            dma((2, SENDS)),
            dma((2, LANDINGS)),
            dma((STAGES,)),
            dma((2, PACKETS)),
        ],
        compiler_params=pltpu.CompilerParams(
            collective_id=collective_id, has_side_effects=True, vmem_limit_bytes=67043328
        ),
        name="move",
    )(idx, out_idx, gate.reshape(cut), up.reshape(cut), down.reshape(cut))
    return tuple(m.reshape(gate.shape) for m in moved)
PIECES = 4


def token_kernel(chips, experts, blocks, old_ref, tokens, ids_ref, logits_ref, gate, up, down, result,
                 rows_all, gate_up, downs, hidden, inbox, outbox, own_sems, pair_sems, ag_send, ag_recv, rs_send, rs_recv):
    half = chips // 2
    count, width = tokens.shape
    feats = gate.shape[1]
    cols = width // PIECES
    tail = rows_all.shape[2] - width
    me = lax.axis_index("expert")
    chip, core = me // 2, me % 2
    mate = {"expert": me + 1 - 2 * core}
    ways = ({"expert": ((chip + 1) % chips) * 2 + core}, {"expert": ((chip + chips - 1) % chips) * 2 + core})
    mesh_ids = pl.DeviceIdType.MESH

    lane = lax.broadcasted_iota(jnp.int32, (count, tail), 1)
    first, second = logits_ref[:, 0:1], logits_ref[:, 1:2]
    weight0 = 1.0 / (1.0 + jnp.exp(second - first))
    weight1 = 1.0 / (1.0 + jnp.exp(first - second))
    which = lane % experts
    value = jnp.where(which == ids_ref[:, 0:1], weight0, jnp.where(which == ids_ref[:, 1:2], weight1, 0.0))
    high = value.astype(jnp.bfloat16).astype(jnp.float32)
    middle = (value - high).astype(jnp.bfloat16).astype(jnp.float32)
    low = value - high - middle
    part = lane // experts
    routed = jnp.where(part == 0, high, jnp.where(part == 1, middle, jnp.where(part == 2, low, 0.0)))
    rows_all[chip, :, width:] = routed.astype(jnp.bfloat16)

    rows_all[chip, :, pl.ds(0, width)] = tokens[...]
    loads = []
    for a, (array, target) in enumerate(
        (
            (gate, gate_up.at[core, :, pl.ds(0, feats)]),
            (up, gate_up.at[core, :, pl.ds(feats, feats)]),
            (down, downs.at[core]),
        )
    ):
        kept = pltpu.make_async_copy(array, target, own_sems.at[a])
        kept.start()
        given = pltpu.make_async_remote_copy(
            src_ref=array, dst_ref=target, send_sem=pair_sems.at[0, a], recv_sem=pair_sems.at[1, a],
            device_id=mate, device_id_type=mesh_ids,
        )
        loads.append((kept, given))

    barrier = pltpu.get_barrier_semaphore()
    for other in (mate,) + ways:
        pl.semaphore_signal(barrier, inc=1, device_id=other, device_id_type=mesh_ids)
    pl.semaphore_wait(barrier, 3)

    def span(p):
        return pl.ds(p * cols, cols + (tail if p == PIECES - 1 else 0))

    def around(offset):
        return lax.rem(chip + offset + 2 * chips, chips)

    def pass_on(way, step, p):
        at = around(1 - step if way == 0 else step - 1)
        view = rows_all.at[at, :, span(p)]
        return pltpu.make_async_remote_copy(
            src_ref=view, dst_ref=view, send_sem=ag_send.at[way, step % 2, p], recv_sem=ag_recv.at[way, step % 2, p],
            device_id=ways[way], device_id_type=mesh_ids,
        )

    def landed(way, step, p):
        at = around(-step if way == 0 else step)
        view = rows_all.at[at, :, span(p)]
        return pltpu.make_async_remote_copy(
            src_ref=view, dst_ref=view, send_sem=ag_send.at[way, step % 2, p], recv_sem=ag_recv.at[way, step % 2, p],
            device_id=ways[way], device_id_type=mesh_ids,
        )

    def shares(way, p):
        return (p < PIECES // 2) == (way == 0)

    def group_rows(g, p):
        view = pl.ds(p * cols, cols)
        if isinstance(g, int) and g in (0, half):
            return rows_all[around(g), :, view]
        return jnp.concatenate([rows_all[around(-g), :, view], rows_all[around(g), :, view]], axis=0)

    def project(g, p, sums):
        x = group_rows(g, p)
        return [
            sums[q] + jnp.dot(x, gate_up[q, pl.ds(p * cols, cols), :], preferred_element_type=jnp.float32)
            for q in range(2)
        ]

    def activate(g, sums):
        for q in range(2):
            g_val, u_val = sums[q][:, :feats], sums[q][:, feats:]
            h = (g_val / (1.0 + jnp.exp(-g_val)) * u_val).astype(jnp.bfloat16)
            if isinstance(g, int) and g in (0, half):
                hidden[around(g), q] = h
            else:
                hidden[around(-g), q] = h[:count]
                hidden[around(g), q] = h[count:]

    def zeros(g):
        m = count if isinstance(g, int) and g in (0, half) else 2 * count
        return [jnp.zeros((m, 2 * feats), jnp.float32) for _ in range(2)]

    def whole(g):
        sums = zeros(g)
        for p in range(PIECES):
            sums = project(g, p, sums)
        activate(g, sums)

    for p in range(PIECES):
        for way in range(2):
            pass_on(way, 1, p).start()
    for _, given in loads:
        given.start()

    def ag_step(step, g, reuse, last):
        sums = None if g is None else zeros(g)
        for p in range(PIECES):
            for way in range(2):
                landed(way, step, p).wait_recv()
            for way in range(2):
                if not last or shares(way, p):
                    if reuse:
                        pass_on(way, step - 1, p).wait_send()
                    pass_on(way, step + 1, p).start()
            if g is not None:
                sums = project(g, p, sums)
        if g is not None:
            activate(g, sums)

    def weights_in():
        for kept, given in loads:
            kept.wait()
            given.wait()

    for step in range(1, min(3, half)):
        if step == 2:
            weights_in()
        ag_step(step, None if step == 1 else 0, step > 1, step == half - 1)
    if half > 4:

        def ag_body(step, carry):
            ag_step(step, step - 2, True, False)
            return carry

        lax.fori_loop(3, half - 1, ag_body, 0)
    if half > 3:
        ag_step(half - 1, half - 3, True, True)
    if half < 3:
        weights_in()
    for p in range(PIECES):
        for way in range(2):
            if shares(way, p):
                landed(way, half, p).wait_recv()
    whole(half)
    done = [g for g in range(half) if not (g <= half - 3)]

    slot0, slot1 = jnp.int32(0), jnp.int32(0)
    for s in range(2 * chips):
        slot0 = slot0 + jnp.where(old_ref[s] == 2 * chip, s // blocks, 0)
        slot1 = slot1 + jnp.where(old_ref[s] == 2 * chip + 1, s // blocks, 0)

    def factors(at):
        extra = rows_all[at, :, width:].astype(jnp.float32)
        lanes = lax.broadcasted_iota(jnp.int32, (count, tail), 1)
        return [
            jnp.sum(jnp.where((lanes % experts == s) & (lanes < 3 * experts), extra, 0.0), axis=1, keepdims=True)
            for s in (slot0, slot1)
        ]

    def contribution(h, f, p):
        total = None
        for q in range(2):
            value = lax.dot_general(
                h[q], downs[q, pl.ds(p * cols, cols), :], (((1,), (1,)), ((), ())), preferred_element_type=jnp.float32
            )
            value = f[q] * value
            total = value if total is None else total + value
        return total

    def both(step):
        owners = (around(half - step + 1), around(step - 1 - half))
        h = [jnp.concatenate([hidden[o, q] for o in owners], axis=0) for q in range(2)]
        fs = [factors(o) for o in owners]
        return h, [jnp.concatenate([fs[0][q], fs[1][q]], axis=0) for q in range(2)]

    def send_on(way, step, p):
        return pltpu.make_async_remote_copy(
            src_ref=outbox.at[way, step % 2, p], dst_ref=inbox.at[way, step % 2, p],
            send_sem=rs_send.at[way, step % 2, p], recv_sem=rs_recv.at[way, step % 2, p],
            device_id=ways[way], device_id_type=mesh_ids,
        )

    def rs_step(step, first, second, reuse):
        h, f = both(step)
        for p in range(PIECES):
            value = contribution(h, f, p)
            sent = [way for way in range(2) if not first or shares(way, p)]
            met = [way for way in range(2) if not first and (not second or shares(way, p))]
            for way in met:
                send_on(way, step - 1, p).wait_recv()
            mine = [value[way * count:(way + 1) * count] for way in range(2)]
            for way in met:
                mine[way] = mine[way] + inbox[way, (step - 1) % 2, p].astype(jnp.float32)
            for way in sent:
                if reuse is True or (reuse == "part" and shares(way, p)):
                    send_on(way, step - 2, p).wait_send()
                outbox[way, step % 2, p] = mine[way].astype(jnp.bfloat16)
            for way in sent:
                send_on(way, step, p).start()

    rs_step(1, True, False, False)
    for g in done:
        whole(g)
    if half > 1:
        rs_step(2, False, True, False)
    if half > 2:
        rs_step(3, False, False, "part")
    if half > 3:

        def rs_body(step, carry):
            rs_step(step, False, False, True)
            return carry

        lax.fori_loop(4, half + 1, rs_body, 0)
    h = [hidden[chip, q] for q in range(2)]
    f = factors(chip)
    for p in range(PIECES):
        value = contribution(h, f, p)
        for way in range(2):
            send_on(way, half, p).wait_recv()
            value = value + inbox[way, half % 2, p].astype(jnp.float32)
        result[:, pl.ds(p * cols, cols)] = value.astype(jnp.bfloat16)
    for p in range(PIECES):
        for way in range(2):
            for step in range(max(1, half - 1), half + 1):
                if step > 1 or shares(way, p):
                    send_on(way, step, p).wait_send()
            final = half if shares(way, p) else half - 1
            for step in range(max(1, final - 1), final + 1):
                pass_on(way, step, p).wait_send()


def token_layer(old_place, tokens, ids, logits, gate, up, down, chips, collective_id):
    count, width = tokens.shape
    feats = gate.shape[2]
    cols = width // PIECES
    any_space = pl.BlockSpec(memory_space=pl.ANY)
    smem = pl.BlockSpec(memory_space=pltpu.SMEM)
    vmem = pl.BlockSpec(memory_space=pltpu.VMEM)
    dma = pltpu.SemaphoreType.DMA
    weights = [w.reshape(w.shape[1:]) for w in (gate, up, down)]
    return pl.pallas_call(
        functools.partial(token_kernel, chips, EXPERTS, 2 * chips // EXPERTS),
        out_shape=jax.ShapeDtypeStruct(tokens.shape, tokens.dtype),
        in_specs=[smem, vmem, vmem, vmem, any_space, any_space, any_space],
        out_specs=vmem,
        scratch_shapes=[
            pltpu.VMEM((chips, count, width + LANES), tokens.dtype),
            pltpu.VMEM((2, width, 2 * feats), tokens.dtype),
            pltpu.VMEM((2, width, feats), tokens.dtype),
            pltpu.VMEM((chips, 2, count, feats), tokens.dtype),
            pltpu.VMEM((2, 2, PIECES, count, cols), tokens.dtype),
            pltpu.VMEM((2, 2, PIECES, count, cols), tokens.dtype),
            dma((3,)),
            dma((2, 3)),
            dma((2, 2, PIECES)),
            dma((2, 2, PIECES)),
            dma((2, 2, PIECES)),
            dma((2, 2, PIECES)),
        ],
        compiler_params=pltpu.CompilerParams(
            collective_id=collective_id, has_side_effects=True, vmem_limit_bytes=67043328
        ),
        name="token_layer",
    )(old_place, tokens, ids, logits, *weights)


def in_one_piece(arrays, axis, split_dim, concat_dim, along):
    both = jnp.concatenate(arrays, axis=along)
    out, at, gathered = (
        lax.all_to_all(both, axis, split_axis=split_dim, concat_axis=concat_dim, tiled=True),
        0,
        [],
    )
    for a in arrays:
        gathered.append(lax.slice_in_dim(out, at, at + a.shape[along], axis=along))
        at += a.shape[along]
    return tuple(gathered)


LIMIT = 144
STEPS = (108, 116, 124, 132, 144)


def two_exchanges(source_of, held_gate, held_up, held_down):
    pieces = in_one_piece((held_gate, held_up, held_down), "expert", 1, 0, 2)
    reordered = tuple(jnp.take(p, source_of, axis=0) for p in pieces)
    return in_one_piece(reordered, "expert", 0, 1, 2)


def migrate(old_place, new_place, slot_new_at, held_gate, held_up, held_down):
    chips = lax.axis_size("expert") // 2
    source_of = jnp.take(old_place, slot_new_at)
    idx, out_idx, info = plan(old_place, new_place, chips, LIMIT)
    fits = [(info[0] <= s) & (info[1] == 0) for s in STEPS]
    choice = len(STEPS) - sum(f.astype(jnp.int32) for f in fits)
    branches = [
        functools.partial(lambda s, i, args: move(args[0], args[1], args[2], args[3], args[4], chips, s, i), s, i)
        for i, s in enumerate(STEPS)
    ]
    branches.append(lambda args: two_exchanges(source_of, args[2], args[3], args[4]))
    return lax.switch(choice, branches, (idx, out_idx, held_gate, held_up, held_down))


def inverse_of(placement, device_ids):
    return jnp.sum(
        jnp.where(placement[:, None] == device_ids[None, :], device_ids[:, None], 0), axis=0
    )


def per_device(
    tokens, route_ids, route_logits, old_place, new_place, held_gate, held_up, held_down
):
    chips = lax.axis_size("expert") // 2
    device_ids = jnp.arange(2 * chips, dtype=jnp.int32)
    moved = migrate(old_place, new_place, inverse_of(new_place, device_ids), held_gate, held_up, held_down)
    output = token_layer(
        old_place, tokens, route_ids, route_logits, held_gate, held_up, held_down, chips, len(STEPS)
    )
    return (output,) + tuple(moved)


def solution(mesh):
    placed = (
        P(("groups", "expert"), None),
        P(("groups", "expert"), None),
        P(("groups", "expert"), None),
        P(),
        P(),
        P(("groups", "expert"), None, None),
        P(("groups", "expert"), None, None),
        P(("groups", "expert"), None, None),
    )
    return jax.shard_map(
        per_device,
        mesh=mesh,
        in_specs=placed,
        out_specs=(
            P(("groups", "expert"), None),
            P(("groups", "expert"), None, None),
            P(("groups", "expert"), None, None),
            P(("groups", "expert"), None, None),
        ),
        check_vma=False,
    )
```

```python
import functools

import jax
import jax.numpy as jnp
from jax import lax
from jax.experimental import pallas as pl
from jax.experimental.pallas import tpu as pltpu
from jax.sharding import PartitionSpec as P

EXPERTS = 8
LANES = 128
PIECES = 4
PACKETS = 12
LAG = 2
LANDINGS = 4
SENDS = 3
STAGES = 4
STEPS = (104, 110, 116, 122, 128, 134, 146)
LIMIT = STEPS[-1]
ROUNDS = 48
BETA = 2.0 * 0.6931472
RISE = 4.0 ** (1.0 / (ROUNDS - 1))
FALL = 0.02 ** (1.0 / (ROUNDS - 1))
TRADES = 16
MESH = pl.DeviceIdType.MESH


def column(row, size):
    r = lax.broadcasted_iota(jnp.int32, (size, size), 0)
    c = lax.broadcasted_iota(jnp.int32, (size, size), 1)
    return jnp.sum(jnp.where(r == c, jnp.broadcast_to(row, (size, size)), 0), axis=1, keepdims=True)


def pick(mask, values):
    return jnp.sum(jnp.where(mask, values, 0.0), axis=0, keepdims=True)


class Plan:
    def __init__(self, chips, chip, old_ref, new_ref, table_ref, choice_ref, fixed, live, small, sched):
        self.chips, self.chip, self.slots = chips, chip, 2 * chips
        self.old_ref, self.new_ref, self.table_ref, self.choice_ref = old_ref, new_ref, table_ref, choice_ref
        self.fixed, self.live, self.small, self.sched = fixed, live, small, sched
        self.rows = sched.shape[0]

    def lanes(self):
        return lax.broadcasted_iota(jnp.int32, (self.slots, LANES), 1)

    def start(self):
        chips, slots = self.chips, self.slots
        old, new = column(self.old_ref[...], slots), column(self.new_ref[...], slots)
        src, dst = old // 2, new // 2
        lanes = self.lanes()
        upward = lanes < chips
        spot = jnp.where(upward, lanes, lanes - chips)
        ahead = dst - src
        ahead = jnp.where(ahead < 0, ahead + chips, ahead)
        back = jnp.where(ahead == 0, 0, chips - ahead)
        origin = jnp.where(upward, src, jnp.where(src == 0, 0, chips - src))
        gone = spot - origin
        gone = jnp.where(gone < 0, gone + chips, gone)
        length = jnp.where(upward, ahead, back)
        here = (lanes < slots) & (gone < length)
        left = jnp.where(here, length - gone, 0).astype(jnp.float32)
        first = here & (gone == 0)
        ids = lax.broadcasted_iota(jnp.int32, (slots, LANES), 0).astype(jnp.float32)
        key = jnp.where(here, left * slots + ids, -3.0)
        one, wrapped = pltpu.roll(key, 1, 1), pltpu.roll(key, LANES - (chips - 1), 1)
        behind = jnp.where((lanes == 0) | (lanes == chips), wrapped, one)
        self.fixed[0] = jnp.where(here, 1.0, 0.0)
        self.fixed[1] = key
        self.fixed[2] = jnp.where(here & ~first, behind, -2.0)
        self.fixed[3] = jnp.where(first, 1.0, 0.0)
        ups = ahead.astype(jnp.float32)
        self.live[0] = jnp.broadcast_to(jnp.clip(0.5 + (0.5 * chips - ups) * 0.25, 0.0, 1.0), (slots, LANES))
        self.small[...] = jnp.full(self.small.shape, -1.0, jnp.float32)
        self.sched[...] = jnp.full(self.sched.shape, -1.0, jnp.float32)

    def price(self, x, total, beta):
        on = self.fixed[0]
        share = jnp.where(self.lanes() < self.chips, x, total - x)
        load = jnp.sum(share * on, axis=0, keepdims=True)
        top = jnp.max(load, axis=1, keepdims=True)
        lane = lax.broadcasted_iota(jnp.int32, (1, LANES), 1)
        return jnp.where(lane < self.slots, jnp.exp(beta * (load - top)), 0.0)

    def descend(self, i):
        i = jnp.asarray(i, jnp.int32).astype(jnp.float32) * jnp.ones((1, 1), jnp.float32)
        beta = BETA * jnp.exp(i * jnp.log(jnp.float32(RISE)))
        step = jnp.exp(i * jnp.log(jnp.float32(FALL)))
        x, on = self.live[0], self.fixed[0]
        price = self.price(x, 1.0, beta)
        total = jnp.sum(price, axis=1, keepdims=True)
        gain = jnp.sum(jnp.where(self.lanes() < self.chips, -on, on) * price, axis=1, keepdims=True)
        self.live[0] = jnp.clip(x + step * (gain / total), 0.0, 1.0)

    def settle(self):
        self.live[0] = jnp.floor(self.live[0] * PACKETS + 0.5)

    def trade(self):
        u, on = self.live[0], self.fixed[0]
        price = self.price(u, float(PACKETS), 0.6931472) * on
        upward = self.lanes() < self.chips
        lower = jnp.sum(jnp.where(upward, -0.5, 1.0) * price, axis=1, keepdims=True)
        higher = jnp.sum(jnp.where(upward, 1.0, -0.5) * price, axis=1, keepdims=True)
        units = u[:, 0:1]
        moves = jnp.sum(on, axis=1, keepdims=True) > 0
        lower = jnp.where(moves & (units > 0), lower, 1e9)
        higher = jnp.where(moves & (units < PACKETS), higher, 1e9)
        best = jnp.minimum(lower, higher)
        least = jnp.min(best, axis=0, keepdims=True)
        ids = lax.broadcasted_iota(jnp.int32, (self.slots, 1), 0).astype(jnp.float32)
        chosen = jnp.min(jnp.where(best == least, ids, 1e9), axis=0, keepdims=True)
        turn = (ids == chosen) & (least < 0)
        self.live[0] = u + jnp.where(turn, jnp.where(lower < higher, -1.0, 1.0), 0.0)

    def load(self):
        u = self.live[0]
        self.live[1] = self.fixed[3] * jnp.where(self.lanes() < self.chips, u, PACKETS - u)

    def send(self, t):
        key, before, count, came = self.fixed[1], self.fixed[2], self.live[1], self.small[0]
        ready = count > 0
        best = jnp.max(jnp.where(ready, key, -1.0), axis=0, keepdims=True)
        self.live[1] = (
            count - jnp.where(ready & (key == best), 1.0, 0.0) + jnp.where(before == came[0:1], 1.0, 0.0)
        )
        wide = jnp.broadcast_to(best, came.shape)
        slot = jnp.where(wide < 0, -1.0, wide - self.slots * jnp.floor(wide / self.slots))
        self.sched[pl.ds(t, 1), :] = slot[0:1]
        self.small[1] = jnp.where(wide >= 0, jnp.asarray(t, jnp.int32).astype(jnp.float32), self.small[1])
        one, wrapped = pltpu.roll(wide, 1, 1), pltpu.roll(wide, LANES - (self.chips - 1), 1)
        lane = lax.broadcasted_iota(jnp.int32, came.shape, 1)
        self.small[0] = jnp.where((lane == 0) | (lane == self.chips), wrapped, one)

    def held(self):
        ids = lax.broadcasted_iota(jnp.int32, (self.slots, 1), 0).astype(jnp.float32)
        old = column(self.old_ref[...], self.slots)
        return [pick(old == 2 * self.chip + q, ids) for q in range(2)]

    def finish(self):
        chips, chip, slots, rows = self.chips, self.chip, self.slots, self.rows
        tall = -(-LIMIT // 8) * 8
        left = self.live[1] + jnp.where(self.fixed[2] == self.small[0, 0:1], 1.0, 0.0)
        used = jnp.max(self.small[1]) + 1.0
        choice = jnp.int32(0)
        for s in STEPS:
            choice = choice + jnp.where(used > s, 1, 0)
        self.choice_ref[0] = jnp.where(jnp.max(left) > 0, len(STEPS), choice)

        table = self.sched[...]
        turned = jnp.concatenate(
            [jnp.transpose(table[k * LANES:(k + 1) * LANES]) for k in range(rows // LANES)], axis=1
        )
        table = table[:tall]
        lane = lax.broadcasted_iota(jnp.int32, (tall, LANES), 1)
        line = lax.broadcasted_iota(jnp.int32, (LANES, rows), 0)
        early = lax.broadcasted_iota(jnp.int32, (tall, rows), 0)
        late = lax.broadcasted_iota(jnp.int32, (tall, rows), 1)
        mirror = jnp.where(chip == 0, 0, chips - chip)
        ends = (
            (chip, jnp.where(chip == 0, chips - 1, chip - 1)),
            (chips + mirror, chips + jnp.where(mirror == 0, chips - 1, mirror - 1)),
        )
        ids = lax.broadcasted_iota(jnp.int32, (slots, 1), 0).astype(jnp.float32)
        old, new = column(self.old_ref[...], slots), column(self.new_ref[...], slots)
        units = self.live[0][:, 0:1]

        held = self.held()
        due = [pick(new == 2 * chip + q, ids) for q in range(2)]
        place = lax.broadcasted_iota(jnp.int32, (1, LANES), 1).astype(jnp.float32)
        base = 2.0 * PACKETS
        sends, found = [], [[], []]
        for way, (mine, theirs) in enumerate(ends):
            out = jnp.sum(jnp.where(lane == mine, table, 0.0), axis=1, keepdims=True)
            got = jnp.sum(jnp.where(lane == theirs, table, 0.0), axis=1, keepdims=True)
            out_row = jnp.sum(jnp.where(line == mine, turned, 0.0), axis=0, keepdims=True)
            got_row = jnp.sum(jnp.where(line == theirs, turned, 0.0), axis=0, keepdims=True)
            out_rank = jnp.sum(jnp.where((out_row == out) & (late < early), 1.0, 0.0), axis=1, keepdims=True)
            got_rank = jnp.sum(jnp.where((got_row == got) & (late < early), 1.0, 0.0), axis=1, keepdims=True)
            rank_row = jnp.sum(jnp.where((got_row == got) & (early < late), 1.0, 0.0), axis=0, keepdims=True)
            spots = base + 2.0 * late.astype(jnp.float32) + way
            index = jnp.sum(jnp.where((got_row == out) & (rank_row == out_rank), spots, 0.0), axis=1, keepdims=True)
            for q in range(2):
                skipped = pick(ids == held[q], units) if way else 0.0
                index = jnp.where(out == held[q], q * PACKETS + skipped + out_rank, index)
            sends.append(jnp.where(out < 0, 0.0, index))
            here = base + 2.0 * lax.broadcasted_iota(jnp.int32, (tall, 1), 0).astype(jnp.float32) + way
            for q in range(2):
                wanted = place - (pick(ids == due[q], units) if way else 0.0)
                found[q].append(jnp.sum(jnp.where((got == due[q]) & (got_rank == wanted), here, 0.0), axis=0, keepdims=True))
        both = jnp.where(lane == 0, sends[0], jnp.where(lane == 1, sends[1], 0.0))
        self.table_ref[pl.ds(0, LIMIT), :] = both[:LIMIT].astype(jnp.int32)
        for q in range(2):
            source = pick(ids == due[q], old.astype(jnp.float32)).astype(jnp.int32)
            packets = jnp.where(place < pick(ids == due[q], units), found[q][0], found[q][1])
            stays = (source % 2).astype(jnp.float32) * PACKETS + place
            packets = jnp.where(source // 2 == chip, stays, packets)
            self.table_ref[pl.ds(LIMIT + q, 1), :] = jnp.where(place < PACKETS, packets, 0.0).astype(jnp.int32)


def token_kernel(
    chips, experts, blocks,
    old_ref, new_ref, tokens, ids_ref, logits_ref, gate, up, down,
    result, table, choice, mate_half,
    rows_all, gate_up, downs, hidden, inbox, outbox, fixed, live, small, sched,
    own_sems, pair_sems, half_sems, ag_send, ag_recv, rs_send, rs_recv,
):
    half = chips // 2
    count, width = tokens.shape
    feats = gate.shape[1]
    cols = width // PIECES
    tail = rows_all.shape[2] - width
    me = lax.axis_index("expert")
    chip, core = me // 2, me % 2
    mate = {"expert": me + 1 - 2 * core}
    ways = ({"expert": ((chip + 1) % chips) * 2 + core}, {"expert": ((chip + chips - 1) % chips) * 2 + core})
    plan = Plan(chips, chip, old_ref, new_ref, table, choice, fixed, live, small, sched)

    lane = lax.broadcasted_iota(jnp.int32, (count, tail), 1)
    first, second = (column(logits_ref[i:i + 1, :], count) for i in range(2))
    expert0, expert1 = (column(ids_ref[i:i + 1, :], count) for i in range(2))
    weight0 = 1.0 / (1.0 + jnp.exp(second - first))
    weight1 = 1.0 / (1.0 + jnp.exp(first - second))
    which = lane % experts
    value = jnp.where(which == expert0, weight0, jnp.where(which == expert1, weight1, 0.0))
    high = value.astype(jnp.bfloat16).astype(jnp.float32)
    middle = (value - high).astype(jnp.bfloat16).astype(jnp.float32)
    low = value - high - middle
    part = lane // experts
    routed = jnp.where(part == 0, high, jnp.where(part == 1, middle, jnp.where(part == 2, low, 0.0)))
    rows_all[chip, :, width:] = routed.astype(jnp.bfloat16)

    rows_all[chip, :, pl.ds(0, width)] = tokens[...]
    loads = []
    for a, (array, target) in enumerate(
        (
            (gate, gate_up.at[core, :, pl.ds(0, feats)]),
            (up, gate_up.at[core, :, pl.ds(feats, feats)]),
            (down, downs.at[core]),
        )
    ):
        kept = pltpu.make_async_copy(array, target, own_sems.at[a])
        kept.start()
        given = pltpu.make_async_remote_copy(
            src_ref=array, dst_ref=target, send_sem=pair_sems.at[0, a], recv_sem=pair_sems.at[1, a],
            device_id=mate, device_id_type=MESH,
        )
        loads.append((kept, given))

    barrier = pltpu.get_barrier_semaphore()
    for other in (mate,) + ways:
        pl.semaphore_signal(barrier, inc=1, device_id=other, device_id_type=MESH)
    pl.semaphore_wait(barrier, 3)

    def span(p):
        return pl.ds(p * cols, cols + (tail if p == PIECES - 1 else 0))

    def around(offset):
        return lax.rem(chip + offset + 2 * chips, chips)

    def pass_on(way, step, p):
        at = around(1 - step if way == 0 else step - 1)
        view = rows_all.at[at, :, span(p)]
        return pltpu.make_async_remote_copy(
            src_ref=view, dst_ref=view, send_sem=ag_send.at[way, step % 2, p], recv_sem=ag_recv.at[way, step % 2, p],
            device_id=ways[way], device_id_type=MESH,
        )

    def landed(way, step, p):
        at = around(-step if way == 0 else step)
        view = rows_all.at[at, :, span(p)]
        return pltpu.make_async_remote_copy(
            src_ref=view, dst_ref=view, send_sem=ag_send.at[way, step % 2, p], recv_sem=ag_recv.at[way, step % 2, p],
            device_id=ways[way], device_id_type=MESH,
        )

    def shares(way, p):
        return (p < PIECES // 2) == (way == 0)

    def group_rows(g, p):
        view = pl.ds(p * cols, cols)
        if isinstance(g, int) and g in (0, half):
            return rows_all[around(g), :, view]
        return jnp.concatenate([rows_all[around(-g), :, view], rows_all[around(g), :, view]], axis=0)

    def project(g, p, sums):
        x = group_rows(g, p)
        return [
            sums[q] + jnp.dot(x, gate_up[q, pl.ds(p * cols, cols), :], preferred_element_type=jnp.float32)
            for q in range(2)
        ]

    def activate(g, sums):
        for q in range(2):
            g_val, u_val = sums[q][:, :feats], sums[q][:, feats:]
            h = (g_val / (1.0 + jnp.exp(-g_val)) * u_val).astype(jnp.bfloat16)
            if isinstance(g, int) and g in (0, half):
                hidden[around(g), q] = h
            else:
                hidden[around(-g), q] = h[:count]
                hidden[around(g), q] = h[count:]

    def zeros(g):
        m = count if isinstance(g, int) and g in (0, half) else 2 * count
        return [jnp.zeros((m, 2 * feats), jnp.float32) for _ in range(2)]

    def whole(g):
        sums = zeros(g)
        for p in range(PIECES):
            sums = project(g, p, sums)
        activate(g, sums)

    for p in range(PIECES):
        for way in range(2):
            pass_on(way, 1, p).start()
    for _, given in loads:
        given.start()

    def chore(step, p):
        at = 4 * (step - 3) + p

        @pl.when(step < 7)
        def _():
            for i in range(ROUNDS // 16):
                plan.descend(at * (ROUNDS // 16) + i)

            if p == PIECES - 1:

                @pl.when(step == 6)
                def _():
                    plan.settle()

        @pl.when((step >= 7) & (step < 9))
        def _():
            for i in range(TRADES // 8):
                plan.trade()

            if p == PIECES - 1:

                @pl.when(step == 8)
                def _():
                    plan.load()

        @pl.when(step >= 9)
        def _():
            for i in range(LIMIT // 24):
                plan.send((at - 24) * (LIMIT // 24) + i)

    def chores():
        def descend(i, carry):
            plan.descend(i)
            return carry

        def trade(i, carry):
            plan.trade()
            return carry

        def send(i, carry):
            plan.send(i)
            return carry

        lax.fori_loop(0, ROUNDS, descend, 0)
        plan.settle()
        lax.fori_loop(0, TRADES, trade, 0)
        plan.load()
        lax.fori_loop(0, LIMIT // 24 * 24, send, 0)

    def ag_step(step, g, reuse, last, between=None):
        sums = None if g is None else zeros(g)
        for p in range(PIECES):
            for way in range(2):
                landed(way, step, p).wait_recv()
            for way in range(2):
                if not last or shares(way, p):
                    if reuse:
                        pass_on(way, step - 1, p).wait_send()
                    pass_on(way, step + 1, p).start()
            if g is not None:
                sums = project(g, p, sums)
            if between is not None:
                between(step, p)
        if g is not None:
            activate(g, sums)

    def weights_in():
        for kept, given in loads:
            kept.wait()
            given.wait()
        for copy in mate_copies():
            copy.start()

    def mate_copies():
        rows = width // 2
        near = pl.ds(core * rows, rows)
        views = (
            gate_up.at[1 - core, near, pl.ds(0, feats)],
            gate_up.at[1 - core, near, pl.ds(feats, feats)],
            downs.at[1 - core, near, :],
        )
        return [pltpu.make_async_copy(v, mate_half.at[a], half_sems.at[a]) for a, v in enumerate(views)]

    steady = half - 4 == 12
    plan.start()
    if not steady:
        chores()
    for step in range(1, min(3, half)):
        if step == 2:
            weights_in()
        ag_step(step, None if step == 1 else 0, step > 1, step == half - 1)
    if half > 4:

        def ag_body(step, carry):
            ag_step(step, step - 2, True, False, chore if steady else None)
            return carry

        lax.fori_loop(3, half - 1, ag_body, 0)
    if half > 3:
        ag_step(half - 1, half - 3, True, True)
    if half < 3:
        weights_in()
    for t in range(LIMIT // 24 * 24, LIMIT):
        plan.send(t)
    plan.finish()
    for p in range(PIECES):
        for way in range(2):
            if shares(way, p):
                landed(way, half, p).wait_recv()
    whole(half)
    done = [g for g in range(half) if not (g <= half - 3)]

    served = [jnp.floor(s / blocks).astype(jnp.int32) for s in plan.held()]

    def factors(at):
        extra = rows_all[at, :, width:].astype(jnp.float32)
        lanes = lax.broadcasted_iota(jnp.int32, (count, tail), 1)
        return [
            jnp.sum(jnp.where((lanes % experts == s) & (lanes < 3 * experts), extra, 0.0), axis=1, keepdims=True)
            for s in served
        ]

    def contribution(h, f, p):
        total = None
        for q in range(2):
            value = lax.dot_general(
                h[q], downs[q, pl.ds(p * cols, cols), :], (((1,), (1,)), ((), ())), preferred_element_type=jnp.float32
            )
            value = f[q] * value
            total = value if total is None else total + value
        return total

    def both(step):
        owners = (around(half - step + 1), around(step - 1 - half))
        h = [jnp.concatenate([hidden[o, q] for o in owners], axis=0) for q in range(2)]
        fs = [factors(o) for o in owners]
        return h, [jnp.concatenate([fs[0][q], fs[1][q]], axis=0) for q in range(2)]

    def send_on(way, step, p):
        return pltpu.make_async_remote_copy(
            src_ref=outbox.at[way, step % 2, p], dst_ref=inbox.at[way, step % 2, p],
            send_sem=rs_send.at[way, step % 2, p], recv_sem=rs_recv.at[way, step % 2, p],
            device_id=ways[way], device_id_type=MESH,
        )

    def rs_step(step, first, second, reuse):
        h, f = both(step)
        for p in range(PIECES):
            value = contribution(h, f, p)
            sent = [way for way in range(2) if not first or shares(way, p)]
            met = [way for way in range(2) if not first and (not second or shares(way, p))]
            for way in met:
                send_on(way, step - 1, p).wait_recv()
            mine = [value[way * count:(way + 1) * count] for way in range(2)]
            for way in met:
                mine[way] = mine[way] + inbox[way, (step - 1) % 2, p].astype(jnp.float32)
            for way in sent:
                if reuse is True or (reuse == "part" and shares(way, p)):
                    send_on(way, step - 2, p).wait_send()
                outbox[way, step % 2, p] = mine[way].astype(jnp.bfloat16)
            for way in sent:
                send_on(way, step, p).start()

    rs_step(1, True, False, False)
    for g in done:
        whole(g)
    if half > 1:
        rs_step(2, False, True, False)
    if half > 2:
        rs_step(3, False, False, "part")
    if half > 3:

        def rs_body(step, carry):
            rs_step(step, False, False, True)
            return carry

        lax.fori_loop(4, half + 1, rs_body, 0)
    for copy in mate_copies():
        copy.wait()
    h = [hidden[chip, q] for q in range(2)]
    f = factors(chip)
    for p in range(PIECES):
        value = contribution(h, f, p)
        for way in range(2):
            send_on(way, half, p).wait_recv()
            value = value + inbox[way, half % 2, p].astype(jnp.float32)
        result[:, pl.ds(p * cols, cols)] = value.astype(jnp.bfloat16)
    for p in range(PIECES):
        for way in range(2):
            for step in range(max(1, half - 1), half + 1):
                if step > 1 or shares(way, p):
                    send_on(way, step, p).wait_send()
            final = half if shares(way, p) else half - 1
            for step in range(max(1, final - 1), final + 1):
                pass_on(way, step, p).wait_send()


def token_layer(old_place, new_place, tokens, ids, logits, gate, up, down, chips, collective_id):
    count, width = tokens.shape
    feats = gate.shape[2]
    cols = width // PIECES
    slots = 2 * chips
    any_space = pl.BlockSpec(memory_space=pl.ANY)
    smem = pl.BlockSpec(memory_space=pltpu.SMEM)
    vmem = pl.BlockSpec(memory_space=pltpu.VMEM)
    dma = pltpu.SemaphoreType.DMA
    weights = [w.reshape(w.shape[1:]) for w in (gate, up, down)]
    return pl.pallas_call(
        functools.partial(token_kernel, chips, EXPERTS, slots // EXPERTS),
        out_shape=(
            jax.ShapeDtypeStruct(tokens.shape, tokens.dtype),
            jax.ShapeDtypeStruct((-(-(LIMIT + 2) // 8) * 8, LANES), jnp.int32),
            jax.ShapeDtypeStruct((1,), jnp.int32),
            jax.ShapeDtypeStruct((3, width // 2, feats), gate.dtype),
        ),
        in_specs=[vmem, vmem, vmem, vmem, vmem, any_space, any_space, any_space],
        out_specs=(vmem, vmem, smem, any_space),
        scratch_shapes=[
            pltpu.VMEM((chips, count, width + LANES), tokens.dtype),
            pltpu.VMEM((2, width, 2 * feats), tokens.dtype),
            pltpu.VMEM((2, width, feats), tokens.dtype),
            pltpu.VMEM((chips, 2, count, feats), tokens.dtype),
            pltpu.VMEM((2, 2, PIECES, count, cols), tokens.dtype),
            pltpu.VMEM((2, 2, PIECES, count, cols), tokens.dtype),
            pltpu.VMEM((4, slots, LANES), jnp.float32),
            pltpu.VMEM((2, slots, LANES), jnp.float32),
            pltpu.VMEM((2, 8, LANES), jnp.float32),
            pltpu.VMEM((2 * LANES, LANES), jnp.float32),
            dma((3,)),
            dma((2, 3)),
            dma((3,)),
            dma((2, 2, PIECES)),
            dma((2, 2, PIECES)),
            dma((2, 2, PIECES)),
            dma((2, 2, PIECES)),
        ],
        compiler_params=pltpu.CompilerParams(
            collective_id=collective_id, has_side_effects=True, vmem_limit_bytes=67043328
        ),
        name="token_layer",
    )(old_place.reshape(1, slots), new_place.reshape(1, slots), tokens, ids.T, logits.T, *weights)


def move_kernel(
    chips, steps, per,
    table, gate, up, down, mate_half,
    new_gate, new_up, new_down,
    pool, landing, sending, stage, load_sems, mate_sem, send_sems, recv_sems, stage_sems, out_sems,
):
    me = lax.axis_index("expert")
    chip, core = me // 2, me % 2
    mate = {"expert": me + 1 - 2 * core}
    above = {"expert": ((chip + 1) % chips) * 2 + core}
    below = {"expert": ((chip + chips - 1) % chips) * 2 + core}
    own_arrays = (gate, up, down)
    new_arrays = (new_gate, new_up, new_down)

    loads = [
        pltpu.make_async_copy(
            array.at[pl.ds(core * per, per)], pool.at[pl.ds(core * PACKETS + a * per, per)], load_sems.at[a]
        )
        for a, array in enumerate(own_arrays)
    ]
    loads.append(pltpu.make_async_copy(mate_half, pool.at[pl.ds((1 - core) * PACKETS, PACKETS)], mate_sem))
    for load in loads:
        load.start()
    barrier = pltpu.get_barrier_semaphore()
    for other in (mate, above, below):
        pl.semaphore_signal(barrier, inc=1, device_id=other, device_id_type=MESH)
    pl.semaphore_wait(barrier, 3)
    for load in loads:
        load.wait()

    def hop(t, way):
        return pltpu.make_async_remote_copy(
            src_ref=sending.at[way, t % SENDS],
            dst_ref=landing.at[way, t % LANDINGS],
            send_sem=send_sems.at[way, t % SENDS],
            recv_sem=recv_sems.at[way, t % LANDINGS],
            device_id=(above, below)[way],
            device_id_type=MESH,
        )

    def take(t):
        for way in range(2):
            hop(t, way).wait_recv()
            pool[2 * PACKETS + 2 * t + way] = landing[way, t % LANDINGS]

    def give(t, free):
        for way in range(2):
            if free:
                hop(t - SENDS, way).wait_send()
            sending[way, t % SENDS] = pool[table[t, way]]
        for way in range(2):
            hop(t, way).start()

    for t in range(SENDS):
        if t >= LAG:
            take(t - LAG)
        give(t, False)

    def body(t, carry):
        take(t - LAG)
        give(t, True)
        return carry

    lax.fori_loop(SENDS, steps, body, 0)
    for t in range(steps - LAG, steps):
        take(t)
    for t in range(steps - SENDS, steps):
        for way in range(2):
            hop(t, way).wait_send()

    def away(p, slot):
        return pltpu.make_async_remote_copy(
            src_ref=stage.at[1, slot],
            dst_ref=new_arrays[p // per].at[core * per + p % per],
            send_sem=out_sems.at[0, slot],
            recv_sem=out_sems.at[1, p],
            device_id=mate,
            device_id_type=MESH,
        )

    def home(p, slot):
        return pltpu.make_async_copy(
            stage.at[0, slot], new_arrays[p // per].at[core * per + p % per], stage_sems.at[slot]
        )

    for p in range(PACKETS):
        slot = p % STAGES
        if p >= STAGES:
            home(p - STAGES, slot).wait()
            away(p - STAGES, slot).wait_send()
        stage[0, slot] = pool[table[LIMIT + core, p]]
        stage[1, slot] = pool[table[LIMIT + 1 - core, p]]
        home(p, slot).start()
        away(p, slot).start()
    for p in range(PACKETS - STAGES, PACKETS):
        home(p, p % STAGES).wait()
        away(p, p % STAGES).wait_send()
    for p in range(PACKETS):
        away(p, p % STAGES).wait_recv()


def move(chips, steps, collective_id, table, gate, up, down, mate_half):
    wide, feats = gate.shape[1], gate.shape[2]
    per = PACKETS // 3
    rows = wide // (2 * per)
    packet = (rows, feats)
    cut = (2 * per, rows, feats)
    any_space = pl.BlockSpec(memory_space=pl.ANY)
    smem = pl.BlockSpec(memory_space=pltpu.SMEM)
    out = jax.ShapeDtypeStruct(cut, gate.dtype)
    dma = pltpu.SemaphoreType.DMA
    moved = pl.pallas_call(
        functools.partial(move_kernel, chips, steps, per),
        out_shape=(out, out, out),
        in_specs=[smem, any_space, any_space, any_space, any_space],
        out_specs=(any_space, any_space, any_space),
        scratch_shapes=[
            pltpu.VMEM((2 * PACKETS + 2 * steps,) + packet, gate.dtype),
            pltpu.VMEM((2, LANDINGS) + packet, gate.dtype),
            pltpu.VMEM((2, SENDS) + packet, gate.dtype),
            pltpu.VMEM((2, STAGES) + packet, gate.dtype),
            dma((3,)),
            dma,
            dma((2, SENDS)),
            dma((2, LANDINGS)),
            dma((STAGES,)),
            dma((2, PACKETS)),
        ],
        compiler_params=pltpu.CompilerParams(
            collective_id=collective_id, has_side_effects=True, vmem_limit_bytes=67043328
        ),
        name="move",
    )(table, gate.reshape(cut), up.reshape(cut), down.reshape(cut), mate_half.reshape((PACKETS,) + packet))
    return tuple(m.reshape(gate.shape) for m in moved)

def in_one_piece(arrays, split_dim, concat_dim):
    both = jnp.concatenate(arrays, axis=2)
    both = lax.all_to_all(both, "expert", split_axis=split_dim, concat_axis=concat_dim, tiled=True)
    return jnp.split(both, len(arrays), axis=2)


def two_exchanges(old_place, new_place, held_gate, held_up, held_down):
    ids = jnp.arange(old_place.shape[0], dtype=jnp.int32)
    slot_at = jnp.sum(jnp.where(new_place[:, None] == ids[None, :], ids[:, None], 0), axis=0)
    source_of = jnp.take(old_place, slot_at)
    bands = in_one_piece((held_gate, held_up, held_down), 1, 0)
    return tuple(in_one_piece([jnp.take(b, source_of, axis=0) for b in bands], 0, 1))


def per_device(
    tokens, route_ids, route_logits, old_place, new_place, held_gate, held_up, held_down
):
    chips = lax.axis_size("expert") // 2
    held = (held_gate, held_up, held_down)
    output, table, choice, mate_half = token_layer(
        old_place, new_place, tokens, route_ids, route_logits, *held, chips, len(STEPS)
    )

    def planned(i, steps, old, new, table, half, *held):
        return move(chips, steps, i, table, *held, half)

    def general(old, new, table, half, *held):
        return two_exchanges(old, new, *held)

    branches = [functools.partial(planned, i, steps) for i, steps in enumerate(STEPS)] + [general]
    moved = lax.switch(choice[0], branches, old_place, new_place, table, mate_half, *held)
    return (output,) + tuple(moved)


def solution(mesh):
    placed = (
        P(("groups", "expert"), None),
        P(("groups", "expert"), None),
        P(("groups", "expert"), None),
        P(),
        P(),
        P(("groups", "expert"), None, None),
        P(("groups", "expert"), None, None),
        P(("groups", "expert"), None, None),
    )
    return jax.shard_map(
        per_device,
        mesh=mesh,
        in_specs=placed,
        out_specs=(
            P(("groups", "expert"), None),
            P(("groups", "expert"), None, None),
            P(("groups", "expert"), None, None),
            P(("groups", "expert"), None, None),
        ),
        check_vma=False,
    )
```

```python
import functools

import jax
import jax.numpy as jnp
from jax import lax
from jax.experimental import pallas as pl
from jax.experimental.pallas import tpu as pltpu
from jax.sharding import PartitionSpec as P

EXPERTS = 8
LANES = 128
PIECES = 4
PACKETS = 12
LAG = 2
LANDINGS = 4
SENDS = 2
STEPS = (103, 109, 115, 121, 127, 140)
LIMIT = STEPS[-1]
LISTED = -(-LIMIT // 28) * 28
ROUNDS = 32
LOG2 = 0.6931472
BETA = 2.0 * LOG2
RISE = 4.0 ** (1.0 / (ROUNDS - 1))
FALL = 0.02 ** (1.0 / (ROUNDS - 1))
TRADES = 24
MESH = pl.DeviceIdType.MESH


def column(row, size):
    r = lax.broadcasted_iota(jnp.int32, (size, size), 0)
    c = lax.broadcasted_iota(jnp.int32, (size, size), 1)
    return jnp.sum(jnp.where(r == c, jnp.broadcast_to(row, (size, size)), 0), axis=1, keepdims=True)


def pick(mask, values):
    return jnp.sum(jnp.where(mask, values, 0.0), axis=0, keepdims=True)


class Plan:
    def __init__(self, chips, chip, old_ref, new_ref, table_ref, choice_ref, fixed, live, small, sched):
        self.chips, self.chip, self.slots = chips, chip, 2 * chips
        self.old_ref, self.new_ref, self.table_ref, self.choice_ref = old_ref, new_ref, table_ref, choice_ref
        self.fixed, self.live, self.small, self.sched = fixed, live, small, sched
        self.rows = sched.shape[0]

    def lanes(self):
        return lax.broadcasted_iota(jnp.int32, (self.slots, LANES), 1)

    def start(self):
        chips, slots = self.chips, self.slots
        old, new = column(self.old_ref[...], slots), column(self.new_ref[...], slots)
        src, dst = old // 2, new // 2
        lanes = self.lanes()
        upward = lanes < chips
        spot = jnp.where(upward, lanes, lanes - chips)
        ahead = dst - src
        ahead = jnp.where(ahead < 0, ahead + chips, ahead)
        back = jnp.where(ahead == 0, 0, chips - ahead)
        origin = jnp.where(upward, src, jnp.where(src == 0, 0, chips - src))
        gone = spot - origin
        gone = jnp.where(gone < 0, gone + chips, gone)
        length = jnp.where(upward, ahead, back)
        here = (lanes < slots) & (gone < length)
        left = jnp.where(here, length - gone, 0).astype(jnp.float32)
        first = here & (gone == 0)
        ids = lax.broadcasted_iota(jnp.int32, (slots, LANES), 0).astype(jnp.float32)
        key = jnp.where(here, left * slots + ids, -3.0)
        one, wrapped = pltpu.roll(key, 1, 1), pltpu.roll(key, LANES - (chips - 1), 1)
        behind = jnp.where((lanes == 0) | (lanes == chips), wrapped, one)
        self.fixed[0] = jnp.where(here, 1.0, 0.0)
        self.fixed[1] = key
        self.fixed[2] = jnp.where(here & ~first, behind, -2.0)
        self.fixed[3] = jnp.where(first, 1.0, 0.0)
        self.fixed[4] = jnp.broadcast_to(jnp.where(ahead > 0, 1.0, 0.0), (slots, LANES))
        ups = ahead.astype(jnp.float32)
        self.live[0] = jnp.broadcast_to(jnp.clip(0.5 + (0.5 * chips - ups) * 0.25, 0.0, 1.0), (slots, LANES))
        self.small[...] = jnp.full(self.small.shape, -1.0, jnp.float32)
        self.sched[...] = jnp.full(self.sched.shape, -1.0, jnp.float32)

    def price(self, x, total, beta, supply=0.0):
        share = jnp.where(self.lanes() < self.chips, x, total - x)
        load = jnp.sum(share * self.fixed[0], axis=0, keepdims=True)
        if supply:
            load = load + jnp.maximum(supply - jnp.sum(share * self.fixed[3], axis=0, keepdims=True), 0.0)
        top = jnp.max(load, axis=1, keepdims=True)
        lane = lax.broadcasted_iota(jnp.int32, (1, LANES), 1)
        return jnp.where(lane < self.slots, jnp.exp(beta * (load - top)), 0.0)

    def descend(self, i):
        i = jnp.asarray(i, jnp.int32).astype(jnp.float32) * jnp.ones((1, 1), jnp.float32)
        beta = BETA * jnp.exp(i * jnp.log(jnp.float32(RISE)))
        step = jnp.exp(i * jnp.log(jnp.float32(FALL)))
        x, on = self.live[0], self.fixed[0]
        price = self.price(x, 1.0, beta)
        total = jnp.sum(price, axis=1, keepdims=True)
        gain = jnp.sum(jnp.where(self.lanes() < self.chips, -on, on) * price, axis=1, keepdims=True)
        self.live[0] = jnp.clip(x + step * (gain / total), 0.0, 1.0)

    def settle(self):
        self.live[0] = jnp.floor(self.live[0] * PACKETS + 0.5)

    def trade(self, i):
        u, on = self.live[0], self.fixed[0]
        price = self.price(u, float(PACKETS), 2.0 * LOG2, float(LAG)) * on
        upward = self.lanes() < self.chips
        lower = jnp.sum(jnp.where(upward, -0.75, 3.0) * price, axis=1, keepdims=True)
        higher = jnp.sum(jnp.where(upward, 3.0, -0.75) * price, axis=1, keepdims=True)
        units = u[:, 0:1]
        moves = self.fixed[4][:, 0:1] > 0
        lower = jnp.where(moves & (units > 0), lower, 1e9)
        higher = jnp.where(moves & (units < PACKETS), higher, 1e9)
        best = jnp.minimum(lower, higher)
        least = jnp.min(best, axis=0, keepdims=True)
        ids = lax.broadcasted_iota(jnp.int32, (self.slots, 1), 0).astype(jnp.float32)
        chosen = jnp.min(jnp.where(best == least, ids, 1e9), axis=0, keepdims=True)
        turn = (ids == chosen) & (least < 0)
        self.live[0] = u + jnp.where(turn, jnp.where(lower < higher, -1.0, 1.0), 0.0)

    def load(self):
        u = self.live[0]
        self.live[1] = self.fixed[3] * jnp.where(self.lanes() < self.chips, u, PACKETS - u)

    def send(self, t):
        key, before, count, came = self.fixed[1], self.fixed[2], self.live[1], self.small[0]
        ready = count > 0
        best = jnp.max(jnp.where(ready, key, -1.0), axis=0, keepdims=True)
        self.live[1] = (
            count - jnp.where(ready & (key == best), 1.0, 0.0) + jnp.where(before == came[0:1], 1.0, 0.0)
        )
        wide = jnp.broadcast_to(best, came.shape)
        slot = jnp.where(wide < 0, -1.0, wide - self.slots * jnp.floor(wide / self.slots))
        self.sched[pl.ds(t, 1), :] = slot[0:1]
        self.small[1] = jnp.where(wide >= 0, jnp.asarray(t, jnp.int32).astype(jnp.float32), self.small[1])
        one, wrapped = pltpu.roll(wide, 1, 1), pltpu.roll(wide, LANES - (self.chips - 1), 1)
        lane = lax.broadcasted_iota(jnp.int32, came.shape, 1)
        self.small[0] = jnp.where((lane == 0) | (lane == self.chips), wrapped, one)

    def held(self):
        ids = lax.broadcasted_iota(jnp.int32, (self.slots, 1), 0).astype(jnp.float32)
        old = column(self.old_ref[...], self.slots)
        return [pick(old == 2 * self.chip + q, ids) for q in range(2)]

    def finish(self):
        chips, chip, slots, rows = self.chips, self.chip, self.slots, self.rows
        tall = -(-LISTED // 8) * 8
        left = self.live[1] + jnp.where(self.fixed[2] == self.small[0, 0:1], 1.0, 0.0)
        used = jnp.max(self.small[1]) + 1.0
        choice = jnp.int32(0)
        for s in STEPS:
            choice = choice + jnp.where(used > s, 1, 0)
        self.choice_ref[0] = jnp.where(jnp.max(left) > 0, len(STEPS), choice)

        table = self.sched[...]
        turned = jnp.concatenate(
            [jnp.transpose(table[k * LANES:(k + 1) * LANES]) for k in range(rows // LANES)], axis=1
        )
        table = table[:tall]
        lane = lax.broadcasted_iota(jnp.int32, (tall, LANES), 1)
        line = lax.broadcasted_iota(jnp.int32, (LANES, rows), 0)
        early = lax.broadcasted_iota(jnp.int32, (tall, rows), 0)
        late = lax.broadcasted_iota(jnp.int32, (tall, rows), 1)
        mirror = jnp.where(chip == 0, 0, chips - chip)
        ends = (
            (chip, jnp.where(chip == 0, chips - 1, chip - 1)),
            (chips + mirror, chips + jnp.where(mirror == 0, chips - 1, mirror - 1)),
        )
        ids = lax.broadcasted_iota(jnp.int32, (slots, 1), 0).astype(jnp.float32)
        old, new = column(self.old_ref[...], slots), column(self.new_ref[...], slots)
        units = self.live[0][:, 0:1]

        held = self.held()
        due = [pick(new == 2 * chip + q, ids) for q in range(2)]
        place = lax.broadcasted_iota(jnp.int32, (1, LANES), 1).astype(jnp.float32)
        base = 2.0 * PACKETS
        sends, found = [], [[], []]
        for way, (mine, theirs) in enumerate(ends):
            out = jnp.sum(jnp.where(lane == mine, table, 0.0), axis=1, keepdims=True)
            got = jnp.sum(jnp.where(lane == theirs, table, 0.0), axis=1, keepdims=True)
            out_row = jnp.sum(jnp.where(line == mine, turned, 0.0), axis=0, keepdims=True)
            got_row = jnp.sum(jnp.where(line == theirs, turned, 0.0), axis=0, keepdims=True)
            out_rank = jnp.sum(jnp.where((out_row == out) & (late < early), 1.0, 0.0), axis=1, keepdims=True)
            got_rank = jnp.sum(jnp.where((got_row == got) & (late < early), 1.0, 0.0), axis=1, keepdims=True)
            rank_row = jnp.sum(jnp.where((got_row == got) & (early < late), 1.0, 0.0), axis=0, keepdims=True)
            spots = base + 2.0 * late.astype(jnp.float32) + way
            index = jnp.sum(jnp.where((got_row == out) & (rank_row == out_rank), spots, 0.0), axis=1, keepdims=True)
            for q in range(2):
                skipped = pick(ids == held[q], units) if way else 0.0
                index = jnp.where(out == held[q], q * PACKETS + skipped + out_rank, index)
            sends.append(jnp.where(out < 0, 0.0, index))
            here = base + 2.0 * lax.broadcasted_iota(jnp.int32, (tall, 1), 0).astype(jnp.float32) + way
            for q in range(2):
                wanted = place - (pick(ids == due[q], units) if way else 0.0)
                found[q].append(jnp.sum(jnp.where((got == due[q]) & (got_rank == wanted), here, 0.0), axis=0, keepdims=True))
        both = jnp.where(lane == 0, sends[0], jnp.where(lane == 1, sends[1], 0.0))
        self.table_ref[pl.ds(0, LIMIT), :] = both[:LIMIT].astype(jnp.int32)
        for q in range(2):
            source = pick(ids == due[q], old.astype(jnp.float32)).astype(jnp.int32)
            packets = jnp.where(place < pick(ids == due[q], units), found[q][0], found[q][1])
            stays = (source % 2).astype(jnp.float32) * PACKETS + place
            packets = jnp.where(source // 2 == chip, stays, packets)
            self.table_ref[pl.ds(LIMIT + q, 1), :] = jnp.where(place < PACKETS, packets, 0.0).astype(jnp.int32)


def gather_kernel(
    chips, experts, blocks,
    old_ref, new_ref, tokens, ids_ref, logits_ref, gate, up, down,
    sums_out, table, choice, mate_half,
    rows_all, gate_up, downs, hidden, sums, fixed, live, small, sched,
    own_sems, pair_sems, half_sems, sum_sems, ag_send, ag_recv,
):
    half = chips // 2
    count, width = tokens.shape
    feats = gate.shape[1]
    cols = width // PIECES
    tail = rows_all.shape[2] - width
    me = lax.axis_index("expert")
    chip, core = me // 2, me % 2
    mate = {"expert": me + 1 - 2 * core}
    ways = ({"expert": ((chip + 1) % chips) * 2 + core}, {"expert": ((chip + chips - 1) % chips) * 2 + core})
    plan = Plan(chips, chip, old_ref, new_ref, table, choice, fixed, live, small, sched)

    loads = []
    for a, (array, target) in enumerate(
        (
            (gate, gate_up.at[core, :, pl.ds(0, feats)]),
            (up, gate_up.at[core, :, pl.ds(feats, feats)]),
            (down, downs.at[core]),
        )
    ):
        kept = pltpu.make_async_copy(array, target, own_sems.at[a])
        kept.start()
        given = pltpu.make_async_remote_copy(
            src_ref=array, dst_ref=target, send_sem=pair_sems.at[0, a], recv_sem=pair_sems.at[1, a],
            device_id=mate, device_id_type=MESH,
        )
        loads.append((kept, given))
    barrier = pltpu.get_barrier_semaphore()
    for other in (mate,) + ways:
        pl.semaphore_signal(barrier, inc=1, device_id=other, device_id_type=MESH)

    lane = lax.broadcasted_iota(jnp.int32, (count, tail), 1)
    first, second = (column(logits_ref[i:i + 1, :], count) for i in range(2))
    expert0, expert1 = (column(ids_ref[i:i + 1, :], count) for i in range(2))
    weight0 = 1.0 / (1.0 + jnp.exp(second - first))
    weight1 = 1.0 / (1.0 + jnp.exp(first - second))
    which = lane % experts
    value = jnp.where(which == expert0, weight0, jnp.where(which == expert1, weight1, 0.0))
    high = value.astype(jnp.bfloat16).astype(jnp.float32)
    middle = (value - high).astype(jnp.bfloat16).astype(jnp.float32)
    low = value - high - middle
    part = lane // experts
    routed = jnp.where(part == 0, high, jnp.where(part == 1, middle, jnp.where(part == 2, low, 0.0)))
    rows_all[chip, :, width:] = routed.astype(jnp.bfloat16)
    rows_all[chip, :, pl.ds(0, width)] = tokens[...]
    pl.semaphore_wait(barrier, 3)

    def span(p):
        return pl.ds(p * cols, cols + (tail if p == PIECES - 1 else 0))

    def around(offset):
        return lax.rem(chip + offset + 2 * chips, chips)

    def passing(at, way, step, p):
        view = rows_all.at[at, :, span(p)]
        return pltpu.make_async_remote_copy(
            src_ref=view, dst_ref=view, send_sem=ag_send.at[way, step % 2, p], recv_sem=ag_recv.at[way, step % 2, p],
            device_id=ways[way], device_id_type=MESH,
        )

    def pass_on(way, step, p):
        return passing(around(1 - step if way == 0 else step - 1), way, step, p)

    def landed(way, step, p):
        return passing(around(-step if way == 0 else step), way, step, p)

    def shares(way, p):
        return (p < PIECES // 2) == (way == 0)

    def owners(batch):
        chips_of = []
        for g in batch:
            one = isinstance(g, int) and g in (0, half)
            chips_of += [around(g)] if one else [around(-g), around(g)]
        return chips_of

    def project(batch, p, totals):
        x = jnp.concatenate([rows_all[o, :, pl.ds(p * cols, cols)] for o in owners(batch)], axis=0)
        return [
            totals[q] + jnp.dot(x, gate_up[q, pl.ds(p * cols, cols), :], preferred_element_type=jnp.float32)
            for q in range(2)
        ]

    def zeros(batch):
        return [jnp.zeros((count * len(owners(batch)), 2 * feats), jnp.float32) for _ in range(2)]

    def activate(batch, totals):
        for q in range(2):
            g_val, u_val = totals[q][:, :feats], totals[q][:, feats:]
            h = (g_val / (1.0 + jnp.exp(-g_val)) * u_val).astype(jnp.bfloat16)
            for i, o in enumerate(owners(batch)):
                hidden[o, q] = h[i * count:(i + 1) * count]

    served = [jnp.floor(s / blocks).astype(jnp.int32) for s in plan.held()]

    def factors(at):
        extra = rows_all[at, :, width:].astype(jnp.float32)
        lanes = lax.broadcasted_iota(jnp.int32, (count, tail), 1)
        return [
            jnp.sum(jnp.where((lanes % experts == s) & (lanes < 3 * experts), extra, 0.0), axis=1, keepdims=True)
            for s in served
        ]

    def leaving(p, i, o):
        return pltpu.make_async_copy(sums.at[p, i], sums_out.at[o, p], sum_sems.at[p, i])

    def scales(batch):
        fs = [factors(o) for o in owners(batch)]
        return [jnp.concatenate([f[q] for f in fs], axis=0) for q in range(2)]

    def expand(batch, p, scale, reused):
        at = owners(batch)
        value = None
        for q in range(2):
            part = lax.dot_general(
                jnp.concatenate([hidden[o, q] for o in at], axis=0), downs[q, pl.ds(p * cols, cols), :],
                (((1,), (1,)), ((), ())), preferred_element_type=jnp.float32,
            )
            part = scale[q] * part
            value = part if value is None else value + part
        for i, o in enumerate(at):

            if isinstance(reused, int):
                if i < reused:
                    leaving(p, i, o).wait()
            else:

                @pl.when(i < reused)
                def _():
                    leaving(p, i, o).wait()

            sums[p, i] = value[i * count:(i + 1) * count]
            leaving(p, i, o).start()

    for p in range(PIECES):
        for way in range(2):
            pass_on(way, 1, p).start()
    for _, given in loads:
        given.start()

    def mate_copies():
        rows = width // 2
        near = pl.ds(core * rows, rows)
        views = (
            gate_up.at[1 - core, near, pl.ds(0, feats)],
            gate_up.at[1 - core, near, pl.ds(feats, feats)],
            downs.at[1 - core, near, :],
        )
        return [pltpu.make_async_copy(v, mate_half.at[a], half_sems.at[a]) for a, v in enumerate(views)]

    def weights_in():
        for kept, given in loads:
            kept.wait()
            given.wait()
        for copy in mate_copies():
            copy.start()

    def repeat(count, what, start=0):
        def body(i, carry):
            what(start + i)
            return carry

        lax.fori_loop(0, count, body, 0)

    def chore(step, p):
        def slot(start):
            return PIECES * (step - start) + p

        if isinstance(step, int) and step < 3:
            repeat(ROUNDS // 8, plan.descend, slot(1) * (ROUNDS // 8))
            if (step, p) == (2, PIECES - 1):
                plan.settle()
            return

        @pl.when(step < 9)
        def _():
            repeat(TRADES // 24, plan.trade)
            if p == PIECES - 1:

                @pl.when(step == 8)
                def _():
                    plan.load()

        @pl.when(step >= 9)
        def _():
            repeat(LISTED // 28, plan.send, slot(9) * (LISTED // 28))

    def chores():
        repeat(ROUNDS, plan.descend)
        plan.settle()
        repeat(TRADES, plan.trade)
        plan.load()
        repeat(LISTED, plan.send)

    def ag_step(step, projected=None, expanded=None, reused=0, between=None, first=False, last=False):
        totals = None if projected is None else zeros(projected)
        scale = None if expanded is None else scales(expanded)
        for p in range(PIECES):
            for way in range(2):
                landed(way, step, p).wait_recv()
            for way in range(2):
                if not last or shares(way, p):
                    if not first:
                        pass_on(way, step - 1, p).wait_send()
                    pass_on(way, step + 1, p).start()

            if projected is not None:
                totals = project(projected, p, totals)
            if expanded is not None:
                expand(expanded, p, scale, reused)
            if between is not None:
                between(step, p)
        if projected is not None:
            activate(projected, totals)

    def whole(batch):
        totals = zeros(batch)
        for p in range(PIECES):
            totals = project(batch, p, totals)
        activate(batch, totals)

    def spread(batch, reused):
        scale = scales(batch)
        for p in range(PIECES):
            expand(batch, p, scale, reused)

    plan.start()
    between = chore if half == 16 else None
    if between is None:
        chores()
    for step in range(1, min(3, half)):
        ag_step(step, between=between, first=step == 1, last=step == half - 1)
    weights_in()
    pairs = max(0, (half - 3) // 2)

    def pair(k, carry):
        batch = (2 * k - 1, 2 * k)
        ag_step(2 * k + 1, projected=batch, between=between)
        ag_step(2 * k + 2, expanded=batch, reused=jnp.where(k > 1, 4, 0), between=between)
        return carry

    lax.fori_loop(1, pairs + 1, pair, 0)
    used = 4 if pairs else 0
    rest = list(range(2 * pairs + 1, half))
    batch = tuple(rest) + (0,)
    if len(rest) > 2:
        ag_step(half - 1, projected=batch, between=between, last=True)
    else:
        whole(batch)
    spread(batch, used)
    used = len(owners(batch))
    plan.finish()
    for p in range(PIECES):
        for way in range(2):
            if shares(way, p):
                landed(way, half, p).wait_recv()
    whole((half,))
    spread((half,), used)
    for p in range(PIECES):
        for i in range(used):
            leaving(p, i, chip).wait()
    for copy in mate_copies():
        copy.wait()
    for p in range(PIECES):
        for way in range(2):
            final = half if shares(way, p) else half - 1
            for step in range(max(1, final - 1), final + 1):
                pass_on(way, step, p).wait_send()


def gather_layer(old_place, new_place, tokens, ids, logits, gate, up, down, chips, collective_id):
    count, width = tokens.shape
    feats = gate.shape[2]
    cols = width // PIECES
    slots = 2 * chips
    any_space = pl.BlockSpec(memory_space=pl.ANY)
    smem = pl.BlockSpec(memory_space=pltpu.SMEM)
    vmem = pl.BlockSpec(memory_space=pltpu.VMEM)
    dma = pltpu.SemaphoreType.DMA
    weights = [w.reshape(w.shape[1:]) for w in (gate, up, down)]
    return pl.pallas_call(
        functools.partial(gather_kernel, chips, EXPERTS, slots // EXPERTS),
        out_shape=(
            jax.ShapeDtypeStruct((chips, PIECES, count, cols), jnp.float32),
            jax.ShapeDtypeStruct((-(-(LIMIT + 2) // 8) * 8, LANES), jnp.int32),
            jax.ShapeDtypeStruct((1,), jnp.int32),
            jax.ShapeDtypeStruct((3, width // 2, feats), gate.dtype),
        ),
        in_specs=[vmem, vmem, vmem, vmem, vmem, any_space, any_space, any_space],
        out_specs=(any_space, vmem, smem, any_space),
        scratch_shapes=[
            pltpu.VMEM((chips, count, width + LANES), tokens.dtype),
            pltpu.VMEM((2, width, 2 * feats), tokens.dtype),
            pltpu.VMEM((2, width, feats), tokens.dtype),
            pltpu.VMEM((chips, 2, count, feats), tokens.dtype),
            pltpu.VMEM((PIECES, 7, count, cols), jnp.float32),
            pltpu.VMEM((5, slots, LANES), jnp.float32),
            pltpu.VMEM((2, slots, LANES), jnp.float32),
            pltpu.VMEM((2, 8, LANES), jnp.float32),
            pltpu.VMEM((2 * LANES, LANES), jnp.float32),
            dma((3,)),
            dma((2, 3)),
            dma((3,)),
            dma((PIECES, 7)),
            dma((2, 2, PIECES)),
            dma((2, 2, PIECES)),
        ],
        compiler_params=pltpu.CompilerParams(
            collective_id=collective_id, has_side_effects=True, vmem_limit_bytes=67043328
        ),
        name="gather_layer",
    )(old_place.reshape(1, slots), new_place.reshape(1, slots), tokens, ids.T, logits.T, *weights)


def move_kernel(
    chips, steps, per,
    table, gate, up, down, mate_half, sums,
    new_gate, new_up, new_down, result,
    pool, landing, sending, stage, inbox, outbox, sum_tiles, total,
    load_sems, mate_sem, send_sems, recv_sems, stage_sems, out_sems, sum_sems, rs_send, rs_recv, result_sem,
):
    half = chips // 2
    me = lax.axis_index("expert")
    chip, core = me // 2, me % 2
    mate = {"expert": me + 1 - 2 * core}
    above = {"expert": ((chip + 1) % chips) * 2 + core}
    below = {"expert": ((chip + chips - 1) % chips) * 2 + core}
    own_arrays = (gate, up, down)
    new_arrays = (new_gate, new_up, new_down)

    loads = [
        pltpu.make_async_copy(
            array.at[pl.ds(core * per, per)], pool.at[pl.ds(core * PACKETS + a * per, per)], load_sems.at[a]
        )
        for a, array in enumerate(own_arrays)
    ]
    loads.append(pltpu.make_async_copy(mate_half, pool.at[pl.ds((1 - core) * PACKETS, PACKETS)], mate_sem))
    for load in loads:
        load.start()
    def around(offset):
        return lax.rem(chip + offset + 2 * chips, chips)

    def relay(way, turn, p):
        return pltpu.make_async_remote_copy(
            src_ref=outbox.at[way, turn, p], dst_ref=inbox.at[way, turn, p],
            send_sem=rs_send.at[way, turn, p], recv_sem=rs_recv.at[way, turn, p],
            device_id=(above, below)[way], device_id_type=MESH,
        )

    def fetch(step, p):
        return [
            pltpu.make_async_copy(sums.at[owner, p], sum_tiles.at[way, p], sum_sems.at[way, p])
            for way, owner in enumerate((around(half - step + 1), around(step - 1 - half)))
        ]

    for t in range(2):
        for copy in fetch(1, t):
            copy.start()
    barrier = pltpu.get_barrier_semaphore()
    for other in (mate, above, below):
        pl.semaphore_signal(barrier, inc=1, device_id=other, device_id_type=MESH)
    pl.semaphore_wait(barrier, 3)
    for load in loads:
        load.wait()

    def hop(way, spot, box):
        return pltpu.make_async_remote_copy(
            src_ref=sending.at[way, spot],
            dst_ref=landing.at[way, box],
            send_sem=send_sems.at[way, spot],
            recv_sem=recv_sems.at[way, box],
            device_id=(above, below)[way],
            device_id_type=MESH,
        )

    def take(t, box):
        for way in range(2):
            hop(way, 0, box).wait_recv()
            pool[2 * PACKETS + 2 * t + way] = landing[way, box]

    def give(t, box, sent):
        spot = t % SENDS
        for way in range(2):
            if sent is True:
                hop(way, spot, box).wait_send()
            else:

                @pl.when(sent)
                def _():
                    hop(way, spot, box).wait_send()

            sending[way, spot] = pool[table[t, way]]
        for way in range(2):
            hop(way, spot, box).start()

    busy = PIECES * half
    head = 3 * PIECES

    def opening(t, carry):
        step, p, box = t // PIECES + 1, t % PIECES, (t + 2) % PIECES
        turn = step % 2

        @pl.when(t >= LAG)
        def _():
            take(t - LAG, box)

        for copy in fetch((t + 2) // PIECES + 1, box):
            copy.start()
        for copy in fetch(step, p):
            copy.wait()
        shared = (p < PIECES // 2, p >= PIECES // 2)
        met = [(step > 2) | ((step == 2) & shared[way]) for way in range(2)]
        for way in range(2):

            @pl.when(met[way])
            def _():
                relay(way, 1 - turn, p).wait_recv()

            @pl.when((step == 3) & shared[way])
            def _():
                relay(way, turn, p).wait_send()

        for way in range(2):

            @pl.when(met[way])
            def _():
                value = sum_tiles[way, p] + inbox[way, 1 - turn, p].astype(jnp.float32)
                outbox[way, turn, p] = value.astype(jnp.bfloat16)

            @pl.when(jnp.logical_not(met[way]) & ((step > 1) | shared[way]))
            def _():
                outbox[way, turn, p] = sum_tiles[way, p].astype(jnp.bfloat16)

        for way in range(2):

            @pl.when((step > 1) | shared[way])
            def _():
                relay(way, turn, p).start()

        give(t, p, t >= SENDS)
        return carry

    def middle(t, carry):
        step, p, box = t // PIECES + 1, t % PIECES, (t + 2) % PIECES
        turn = step % 2
        take(t - LAG, box)
        for copy in fetch((t + 2) // PIECES + 1, box):
            copy.start()
        for copy in fetch(step, p):
            copy.wait()
        for way in range(2):
            relay(way, 1 - turn, p).wait_recv()
            relay(way, turn, p).wait_send()
        for way in range(2):
            value = sum_tiles[way, p] + inbox[way, 1 - turn, p].astype(jnp.float32)
            outbox[way, turn, p] = value.astype(jnp.bfloat16)
        for way in range(2):
            relay(way, turn, p).start()
        give(t, p, True)
        return carry

    def closing(t, carry):
        step, p, box = half + 1, t % PIECES, (t + 2) % PIECES
        turn = step % 2
        take(t - LAG, box)

        @pl.when(t < busy + 2)
        def _():
            for copy in fetch(step, box):
                copy.start()

        for copy in fetch(step, p):
            copy.wait()
        value = sum_tiles[0, p]
        for way in range(2):
            relay(way, 1 - turn, p).wait_recv()
            relay(way, turn, p).wait_send()
        for way in range(2):
            value = value + inbox[way, 1 - turn, p].astype(jnp.float32)
        total[p] = value.astype(jnp.bfloat16)
        give(t, p, True)
        return carry

    def plain(t, carry):
        take(t - LAG, (t + 2) % PIECES)
        give(t, t % PIECES, True)
        return carry

    lax.fori_loop(0, head, opening, 0)
    lax.fori_loop(head, busy, middle, 0)
    lax.fori_loop(busy, busy + PIECES, closing, 0)
    lax.fori_loop(busy + PIECES, steps, plain, 0)
    done = pltpu.make_async_copy(total, result, result_sem)
    done.start()

    for t in range(steps - LAG, steps):
        take(t, t % LANDINGS)
    for way in range(2):
        for p in range(PIECES):
            relay(way, half % 2, p).wait_send()
        for spot in range(SENDS):
            hop(way, spot, 0).wait_send()

    def away(a, i):
        return pltpu.make_async_remote_copy(
            src_ref=stage.at[1, i],
            dst_ref=new_arrays[a].at[core * per + i],
            send_sem=out_sems.at[0, i],
            recv_sem=out_sems.at[1, a * per + i],
            device_id=mate,
            device_id_type=MESH,
        )

    def home(a, i):
        return pltpu.make_async_copy(stage.at[0, i], new_arrays[a].at[core * per + i], stage_sems.at[i])

    for a in range(3):

        def hand_over(i, carry):
            if a > 0:
                home(a - 1, i).wait()
                away(a - 1, i).wait_send()
            stage[0, i] = pool[table[LIMIT + core, a * per + i]]
            stage[1, i] = pool[table[LIMIT + 1 - core, a * per + i]]
            home(a, i).start()
            away(a, i).start()
            return carry

        lax.fori_loop(0, per, hand_over, 0)
    for i in range(per):
        home(2, i).wait()
        away(2, i).wait_send()
    for a in range(3):
        for i in range(per):
            away(a, i).wait_recv()
    done.wait()


def move(chips, steps, collective_id, table, gate, up, down, mate_half, sums):
    wide, feats = gate.shape[1], gate.shape[2]
    per = PACKETS // 3
    rows = wide // (2 * per)
    packet = (rows, feats)
    cut = (2 * per, rows, feats)
    any_space = pl.BlockSpec(memory_space=pl.ANY)
    smem = pl.BlockSpec(memory_space=pltpu.SMEM)
    out = jax.ShapeDtypeStruct(cut, gate.dtype)
    dma = pltpu.SemaphoreType.DMA
    count, cols = sums.shape[2:]
    piece = (PIECES, count, cols)
    return pl.pallas_call(
        functools.partial(move_kernel, chips, steps, per),
        out_shape=(out, out, out, jax.ShapeDtypeStruct(piece, gate.dtype)),
        in_specs=[smem, any_space, any_space, any_space, any_space, any_space],
        out_specs=(any_space, any_space, any_space, any_space),
        scratch_shapes=[
            pltpu.VMEM((2 * PACKETS + 2 * steps,) + packet, gate.dtype),
            pltpu.VMEM((2, LANDINGS) + packet, gate.dtype),
            pltpu.VMEM((2, SENDS) + packet, gate.dtype),
            pltpu.VMEM((2, per) + packet, gate.dtype),
            pltpu.VMEM((2, 2) + piece, gate.dtype),
            pltpu.VMEM((2, 2) + piece, gate.dtype),
            pltpu.VMEM((2, PIECES, count, cols), jnp.float32),
            pltpu.VMEM(piece, gate.dtype),
            dma((3,)),
            dma,
            dma((2, SENDS)),
            dma((2, LANDINGS)),
            dma((per,)),
            dma((2, PACKETS)),
            dma((2, PIECES)),
            dma((2, 2, PIECES)),
            dma((2, 2, PIECES)),
            dma,
        ],
        compiler_params=pltpu.CompilerParams(
            collective_id=collective_id, has_side_effects=True, vmem_limit_bytes=67043328
        ),
        name="move",
    )(table, gate.reshape(cut), up.reshape(cut), down.reshape(cut), mate_half.reshape((PACKETS,) + packet), sums)


def settle_kernel(gate, up, down, pieces, new_gate, new_up, new_down, result, tiles, in_sems, out_sems):
    arrays, outs = (gate, up, down), (new_gate, new_up, new_down)
    parts = tiles.shape[0] // 3
    rows = tiles.shape[1]

    def into(i):
        return pltpu.make_async_copy(arrays[i // parts].at[pl.ds(i % parts * rows, rows)], tiles.at[i], in_sems.at[i])

    def out_of(i):
        return pltpu.make_async_copy(tiles.at[i], outs[i // parts].at[pl.ds(i % parts * rows, rows)], out_sems.at[i])

    for i in range(3 * parts):
        into(i).start()
    cols = pieces.shape[2]
    for p in range(pieces.shape[0]):
        result[:, pl.ds(p * cols, cols)] = pieces[p]
    for i in range(3 * parts):
        into(i).wait()
        out_of(i).start()
    for i in range(3 * parts):
        out_of(i).wait()


def settle(gate, up, down, pieces):
    parts = 1
    wide, feats = gate.shape
    any_space = pl.BlockSpec(memory_space=pl.ANY)
    vmem = pl.BlockSpec(memory_space=pltpu.VMEM)
    dma = pltpu.SemaphoreType.DMA
    out = jax.ShapeDtypeStruct(gate.shape, gate.dtype)
    return pl.pallas_call(
        settle_kernel,
        out_shape=(out, out, out, jax.ShapeDtypeStruct((pieces.shape[1], pieces.shape[0] * pieces.shape[2]), pieces.dtype)),
        in_specs=[any_space, any_space, any_space, vmem],
        out_specs=(any_space, any_space, any_space, vmem),
        scratch_shapes=[
            pltpu.VMEM((3 * parts, wide // parts, feats), gate.dtype),
            dma((3 * parts,)),
            dma((3 * parts,)),
        ],
        compiler_params=pltpu.CompilerParams(vmem_limit_bytes=67043328),
        name="settle",
    )(gate, up, down, pieces)


def in_one_piece(arrays, split_dim, concat_dim):
    both = jnp.concatenate(arrays, axis=2)
    both = lax.all_to_all(both, "expert", split_axis=split_dim, concat_axis=concat_dim, tiled=True)
    return jnp.split(both, len(arrays), axis=2)


def two_exchanges(old_place, new_place, held_gate, held_up, held_down):
    ids = jnp.arange(old_place.shape[0], dtype=jnp.int32)
    slot_at = jnp.sum(jnp.where(new_place[:, None] == ids[None, :], ids[:, None], 0), axis=0)
    source_of = jnp.take(old_place, slot_at)
    bands = in_one_piece((held_gate, held_up, held_down), 1, 0)
    return tuple(in_one_piece([jnp.take(b, source_of, axis=0) for b in bands], 0, 1))


def per_device(
    tokens, route_ids, route_logits, old_place, new_place, held_gate, held_up, held_down
):
    chips = lax.axis_size("expert") // 2
    held = (held_gate, held_up, held_down)
    sums, table, choice, mate_half = gather_layer(
        old_place, new_place, tokens, route_ids, route_logits, *held, chips, len(STEPS)
    )
    flat = held_gate.shape[1:]

    def planned(i, steps, old, new, table, half, sums, *held):
        *moved, pieces = move(chips, steps, i, table, *held, half, sums)
        return tuple(m.reshape(flat) for m in moved) + (pieces,)

    def general(old, new, table, half, sums, *held):
        pieces = move(chips, LIMIT, len(STEPS) - 1, table, *held, half, sums)[3]
        return tuple(m.reshape(flat) for m in two_exchanges(old, new, *held)) + (pieces,)

    branches = [functools.partial(planned, i, steps) for i, steps in enumerate(STEPS)] + [general]
    *moved, pieces = lax.switch(choice[0], branches, old_place, new_place, table, mate_half, sums, *held)
    *moved, output = settle(*moved, pieces)
    return (output,) + tuple(m.reshape(held_gate.shape) for m in moved)


def solution(mesh):
    placed = (
        P(("groups", "expert"), None),
        P(("groups", "expert"), None),
        P(("groups", "expert"), None),
        P(),
        P(),
        P(("groups", "expert"), None, None),
        P(("groups", "expert"), None, None),
        P(("groups", "expert"), None, None),
    )
    return jax.shard_map(
        per_device,
        mesh=mesh,
        in_specs=placed,
        out_specs=(
            P(("groups", "expert"), None),
            P(("groups", "expert"), None, None),
            P(("groups", "expert"), None, None),
            P(("groups", "expert"), None, None),
        ),
        check_vma=False,
    )
```
